256 devices in a mesh: grp: 4 (over y), dev: 64 (over x, z, core).
Axes of the slice: x: 4, y: 4, z: 8, core: 2. Of those that a mesh axis runs over, the one named last changes fastest.
Arguments:
- pool_rows: bfloat16 [262144, 1024], P(('grp', 'dev')), may hold values from -6 to 6
- sample_index: int32 [262144], P(('grp', 'dev')), may hold values from 0 to 262143, as said below
- cluster_id: int32 [262144], P(('grp', 'dev')), may hold values from 0 to 511, as said below
- child_id: int32 [262144], P(('grp', 'dev')), may hold values from 0 to 7
- old_centroids: float32 [512, 8, 1024], P('dev'), may hold values from -6 to 6
Outputs:
- centroids: float32 [512, 8, 1024], P('dev')
- child_counts: int32 [512, 8], P('dev')
The draws below stay inside these ranges and needn't reach their ends.
Inputs may be any that keep to these rules, and one draw needn't show every extreme that they name: Sample i takes a pool row of its own aligned block of 1024 rows: sample_index[i] // 1024 == i // 1024. `cluster_id`: in each aligned block of 1024 samples (the rows of one device) the 2 clusters o * 2 to o * 2 + 1 of any owner o are named at most 8 times together, and one cluster, the same in every block, is named exactly 8 times in every block.
All inputs are finite; a program needn't handle non-finite values.
Results may differ from the reference program's by a relative error of at most 0.0003.
Values may be sent and summed in bfloat16 or wider, within the bound.
No kernel may reach another device: no remote copies, remote signals or barrier semaphores. Data moves between devices by JAX's collectives and lax.ppermute only.
A program may use at most 64 MiB of HBM per device.

```python
import jax
import jax.numpy as jnp
from jax import lax

D = 1024
KC = 8
CL_DEV = 2
R_DEV = 1024
CLUSTERS = 512
ROWS = 262144
MOST = 8


def shuffle_row(subkey, values):
    return jax.random.permutation(subkey, values)


def draw_cluster_id(key, part):
    blocks = ROWS // R_DEV
    holder_tally_overall = CLUSTERS // CL_DEV
    slots = holder_tally_overall * MOST
    full_key = jax.random.fold_in(key, 11)
    favour_noise_seed = jax.random.fold_in(key, 12)
    noise_key = jax.random.fold_in(key, 13)
    order_key = jax.random.fold_in(key, 14)
    pick_key = jax.random.fold_in(key, 15)
    favoured = jax.random.randint(full_key, (), 0, CLUSTERS)
    favourite_holder_position = favoured // CL_DEV
    holder_advantage = jax.random.randint(favour_noise_seed, (holder_tally_overall,), 0, 4)
    uniform_perturbation = jax.random.randint(noise_key, (blocks, slots), 0, 16384)
    holder_table = (jnp.arange(slots) // MOST).astype(jnp.int32)
    holder_merit = uniform_perturbation + holder_advantage[holder_table][None, :] * 4096 + jnp.where(holder_table == favourite_holder_position, 65536, 0)[None, :]
    holder_merit = (holder_merit * slots + jnp.arange(slots)[None, :]).astype(jnp.int32)
    unused, chosen = lax.top_k(holder_merit, R_DEV)
    keys = jax.random.split(order_key, blocks)
    mixed = jax.vmap(shuffle_row)(keys, chosen.astype(jnp.int32))
    owner = (mixed // MOST).astype(jnp.int32)
    pick = jax.random.randint(pick_key, (blocks, R_DEV), 0, CL_DEV)
    cluster = owner * CL_DEV + pick
    cluster = jnp.where(owner == favourite_holder_position, favoured, cluster)
    return cluster.reshape(-1).astype(jnp.int32)


def draw_sample_index(key, part):
    offset_key = jax.random.fold_in(key, 21)
    within = jax.random.randint(offset_key, (ROWS,), 0, R_DEV)
    base = jnp.arange(ROWS) // R_DEV * R_DEV
    return (base + within).astype(jnp.int32)


def place_ends(entries, rng, low, top_value):
    longest = entries.shape.index(max(entries.shape))
    spots = []
    for shift in (0, 1):
        where = [jax.random.randint(jax.random.fold_in(rng, axis), (), 0, length) for axis, length in enumerate(entries.shape)]
        where[longest] = (where[longest] + shift) % entries.shape[longest]
        spots.append(tuple(where))
    return entries.at[spots[0]].set(low).at[spots[1]].set(top_value)


def shard_levels(key, shape, shards, least, largest):
    def one(dim, blocks):
        draws = jax.random.uniform(jax.random.fold_in(jax.random.fold_in(key, 6), dim), (blocks,), jnp.float32, least / len(shards), largest / len(shards))
        return jnp.repeat(jnp.exp(draws), shape[dim] // blocks).reshape((-1,) + (1,) * (len(shape) - dim - 1))

    gain = one(*shards[0])
    for cut in shards[1:]:
        gain = gain * one(*cut)
    return gain


def scatter_about(stream_key, dims, spread, most, pieces=(), dtype=jnp.bfloat16):
    loudness = shard_levels(stream_key, dims, pieces, -0.22, 0.18) if pieces else 1.0
    drawn = jax.random.normal(stream_key, dims, jnp.float32) * spread * loudness
    return jnp.minimum(jnp.maximum(drawn, -most), most).astype(dtype)


def setup_inputs(seed: int = 0) -> dict:
    arg_keys = jax.random.split(jax.random.key(seed), 6)
    pool_rows = scatter_about(arg_keys[0], (ROWS, D), 1.0, 6.0, ((0, 256),))
    sample_index = draw_sample_index(jax.random.fold_in(arg_keys[5], 71), 0)
    cluster_id = draw_cluster_id(jax.random.fold_in(arg_keys[5], 71), 0)
    child_id = place_ends(jax.random.randint(arg_keys[3], (ROWS,), 0, KC), jax.random.fold_in(arg_keys[3], 1), 0, KC - 1).astype(jnp.int32)
    old_centroids = scatter_about(arg_keys[4], (CLUSTERS, KC, D), 1.0, 6.0, ((0, 64),), jnp.float32)
    return dict(pool_rows=pool_rows, sample_index=sample_index, cluster_id=cluster_id, child_id=child_id, old_centroids=old_centroids)


def reference(pool_rows, sample_index, cluster_id, child_id, old_centroids):
    blocks = ROWS // R_DEV
    segments = CLUSTERS * KC

    def add_block(carry, items):
        sums, counts = carry
        index_block, cluster_block, child_block = items
        rows = pool_rows[index_block].astype(jnp.float32)
        segment = (cluster_block * KC + child_block).astype(jnp.int32)
        sums = sums + jax.ops.segment_sum(rows, segment, num_segments=segments)
        ones = jnp.ones(segment.shape, jnp.int32)
        counts = counts + jax.ops.segment_sum(ones, segment, num_segments=segments)
        return (sums, counts), None

    initial = (jnp.zeros((segments, D), jnp.float32), jnp.zeros((segments,), jnp.int32))
    items = (sample_index.reshape(blocks, R_DEV), cluster_id.reshape(blocks, R_DEV), child_id.reshape(blocks, R_DEV))
    (sums, counts), unused = lax.scan(add_block, initial, items)
    child_counts = counts.reshape(CLUSTERS, KC)
    divisor = child_counts.astype(jnp.float32)[:, :, None] + 1.0
    centroids = (sums.reshape(CLUSTERS, KC, D) + old_centroids) / divisor
    return (centroids, child_counts)
```

```python
import functools

import jax
import jax.numpy as jnp
from jax import lax
from jax.experimental import pallas as pl
from jax.experimental.pallas import tpu as pltpu
from jax.sharding import PartitionSpec as P


NY, NX, NZ, NC = 4, 4, 8, 2
LANES = 128
VMEM = pltpu.VMEM
SMEM = pltpu.SMEM


def device_of(y, x, z, c):
    return ((y * NX + x) * NZ + z) * NC + c


def shift(value, dy=0, dx=0, dz=0, dc=0):
    pairs = []
    for y in range(NY):
        for x in range(NX):
            for z in range(NZ):
                for c in range(NC):
                    to = device_of((y + dy) % NY, (x + dx) % NX, (z + dz) % NZ, (c + dc) % NC)
                    pairs.append((device_of(y, x, z, c), to))
    return lax.ppermute(value, ("grp", "dev"), pairs)


def iota(shape, dim):
    return lax.broadcasted_iota(jnp.int32, shape, dim)


def one_hot(mask, dtype=jnp.bfloat16):
    return jnp.where(mask, 1.0, 0.0).astype(dtype)


def dot(a, b, dims=((1,), (0,))):
    return lax.dot_general(a, b, (dims, ((), ())), preferred_element_type=jnp.float32)


def call(kernel, outs, args, scratch=(), limit=40 << 20):
    specs = [
        pl.BlockSpec(memory_space=SMEM if a.dtype == jnp.int32 and a.ndim == 1 and a.size <= 8 else VMEM)
        for a in args
    ]
    return pl.pallas_call(
        kernel,
        out_shape=outs,
        in_specs=specs,
        out_specs=jax.tree.map(lambda _: pl.BlockSpec(memory_space=VMEM), outs),
        scratch_shapes=list(scratch),
        compiler_params=pltpu.CompilerParams(vmem_limit_bytes=limit),
    )(*args)


def ranks(owner, owners):
    rows = owner.shape[1]
    before = one_hot(iota((LANES, LANES), 0) < iota((LANES, LANES), 1))
    ones = jnp.ones((LANES, LANES), jnp.bfloat16)
    seen = jnp.zeros((owners, LANES), jnp.float32)
    out = []
    for b in range(rows // LANES):
        mask = iota((owners, LANES), 0) == owner[:, b * LANES : (b + 1) * LANES]
        hot = one_hot(mask)
        prefix = dot(hot, before) + seen
        seen = seen + dot(hot, ones)
        out.append(jnp.sum(jnp.where(mask, prefix, 0.0), axis=0, keepdims=True))
    return jnp.concatenate(out, axis=1).astype(jnp.int32)


def pack_kernel(most, owned, kinds, where, index_ref, cluster_ref, child_ref, pool_ref, *rest):
    outs, select = rest[:-1], rest[-1]
    y, x = where[0], where[1]
    rows = index_ref.shape[1]
    cluster = cluster_ref[...]
    owner = lax.div(cluster, owned)
    rank = ranks(owner, NY * NX * NZ * NC)
    quarter = lax.rem(owner, NY)
    dev = lax.div(owner, NY)
    to_x = lax.div(dev, NZ * NC)
    to_z = lax.rem(lax.div(dev, NC), NZ)
    to_c = lax.rem(dev, NC)
    chunk = NC * NZ * most
    slot = (quarter * NX + to_x) * chunk + (to_c * NZ + to_z) * most + rank
    label = (to_c * NZ + to_z) * (owned * kinds) + lax.rem(cluster, owned) * kinds + child_ref[...]
    label = jnp.broadcast_to((label + 1).astype(jnp.float32), (8, rows)).astype(jnp.bfloat16)
    index = (index_ref[...] + 1).astype(jnp.float32)
    for j in range(NY * NX):
        dy, dx = j // NX, j % NX
        dest = lax.rem(y + dy, NY) * NX + lax.rem(x + dx, NX)
        mask = iota((chunk, rows), 0) == slot - dest * chunk
        labels = dot(label, one_hot(mask), ((1,), (1,)))
        outs[j][chunk:, :] = jnp.zeros((8, outs[j].shape[1]), jnp.bfloat16)
        outs[j][chunk:, :chunk] = labels.astype(jnp.bfloat16)
        source = jnp.sum(jnp.where(mask, index, 0.0), axis=1, keepdims=True).astype(jnp.int32) - 1
        select[j * chunk : (j + 1) * chunk, :] = one_hot(iota((chunk, rows), 1) == source)
    group = 4
    for g in range(0, NY * NX, group):
        got = dot(select[g * chunk : (g + group) * chunk, :], pool_ref[...]).astype(jnp.bfloat16)
        for j in range(group):
            outs[g + j][:chunk, :] = got[j * chunk : (j + 1) * chunk]


def sum_kernel(where, *rest):
    ins, (mine_ref, other_ref) = rest[:-2], rest[-2:]
    core = where[0]
    half = mine_ref.shape[0]
    width = ins[0].shape[1]
    chunk = ins[0].shape[0] - 8
    row = iota((half, 2 * chunk), 0) + 1
    ones = jnp.ones((2 * chunk, LANES), jnp.bfloat16)
    total = jnp.zeros((2 * half, width), jnp.float32)
    count = jnp.zeros((2 * half, LANES), jnp.float32)
    for j in range(0, len(ins), 2):
        label = jnp.concatenate(
            [r[chunk:, :chunk].astype(jnp.float32)[0:1] for r in ins[j : j + 2]], axis=1
        ).astype(jnp.int32)
        hot = jnp.concatenate(
            [
                one_hot(row == label - core * half),
                one_hot(row == label - (1 - core) * half),
            ],
            axis=0,
        )
        total += dot(hot, jnp.concatenate([r[:chunk, :] for r in ins[j : j + 2]], axis=0))
        count += dot(hot, ones)
    mine_ref[:, :width] = total[:half]
    mine_ref[:, width:] = count[:half]
    other_ref[:, :width] = total[half:]
    other_ref[:, width:] = count[half:]


def split_kernel(where, mine_ref, came_ref, *outs):
    z = where[0]
    part = outs[0].shape[0]
    for j, out in enumerate(outs):
        at = pl.ds(pl.multiple_of(lax.rem(z + j, NZ) * part, part), part)
        out[...] = mine_ref[at, :] + came_ref[at, :]


def finish_kernel(where, old_ref, *rest):
    ins, out = rest[:-1], rest[-1]
    part, width = out.shape[0], old_ref.shape[1]
    at = pl.ds(pl.multiple_of(where[0] * part, part), part)
    total = ins[0][...]
    for r in ins[1:]:
        total = total + r[...]
    count = total[:, width:]
    divisor = jnp.concatenate([count + 1.0] * (width // LANES), axis=1)
    out[:, :width] = (total[:, :width] + old_ref[at, :]) / divisor
    out[:, width:] = count


def place_kernel(where, *rest):
    ins, (fresh_ref, count_ref) = rest[:-2], rest[-2:]
    y = where[0]
    part, width = ins[0].shape[0], fresh_ref.shape[1]
    kinds = count_ref.shape[1]
    pick = iota((part, LANES), 1) == lax.rem(iota((part, LANES), 0), kinds)
    for j, r in enumerate(ins):
        q = lax.rem(y - j + NY, NY)
        fresh_ref[pl.ds(pl.multiple_of(q * part, part), part), :] = r[:, :width]
        count = jnp.where(pick, r[:, width:], 0.0)
        for k in range(part // kinds):
            line = jnp.sum(count[k * kinds : (k + 1) * kinds], axis=0, keepdims=True)
            count_ref[pl.ds(q * (part // kinds) + k, 1), :] = line[:, :kinds].astype(jnp.int32)


def per_device(pool_rows, sample_index, cluster_id, child_id, old_centroids):
    rows, width = pool_rows.shape
    block, kinds = old_centroids.shape[:2]
    owned = block // NY
    most = 4 * rows // (block * NX * NZ * NC)
    chunk = NC * NZ * most
    part = owned * kinds
    y = lax.axis_index("grp")
    dev = lax.axis_index("dev")
    x, z, c = dev // (NZ * NC), dev // NC % NZ, dev % NC

    def shape(*dims, dtype=jnp.float32):
        return jax.ShapeDtypeStruct(dims, dtype)

    lines = [a.reshape(1, rows) for a in (sample_index % rows, cluster_id, child_id)]
    packed = call(
        functools.partial(pack_kernel, most, owned, kinds),
        [shape(chunk + 8, width, dtype=jnp.bfloat16)] * (NY * NX),
        [jnp.stack([y, x]), *lines, pool_rows],
        scratch=[VMEM((NY * NX * chunk, rows), jnp.bfloat16)],
    )
    came = [packed[0]] + [
        shift(packed[j], dy=j // NX, dx=j % NX) for j in range(1, NY * NX)
    ]
    wide = width + LANES
    mine, other = call(
        sum_kernel, [shape(NZ * part, wide)] * 2, [c.reshape(1), *came]
    )
    over = shift(other, dc=1)
    pieces = call(split_kernel, [shape(part, wide)] * NZ, [z.reshape(1), mine, over])
    pieces = [pieces[0]] + [shift(pieces[j], dz=j) for j in range(1, NZ)]
    fresh = call(
        finish_kernel,
        shape(part, wide),
        [y.reshape(1), old_centroids.reshape(block * kinds, width), *pieces],
    )
    quarters = [fresh] + [shift(fresh, dy=j) for j in range(1, NY)]
    centroids, counts = call(
        place_kernel,
        [shape(block * kinds, width), shape(block, kinds, dtype=jnp.int32)],
        [y.reshape(1), *quarters],
    )
    return centroids.reshape(block, kinds, width), counts


def solution(mesh):
    placed = (
        P(("grp", "dev"), None),
        P(("grp", "dev")),
        P(("grp", "dev")),
        P(("grp", "dev")),
        P("dev", None, None),
    )
    return jax.shard_map(
        per_device,
        mesh=mesh,
        in_specs=placed,
        out_specs=(P("dev", None, None), P("dev", None)),
        check_vma=False,
    )
```

```python
import functools

import jax
import jax.numpy as jnp
from jax import lax
from jax.experimental import pallas as pl
from jax.experimental.pallas import tpu as pltpu
from jax.sharding import Mesh, PartitionSpec as P

LANES = 128
VMEM = pltpu.VMEM
SMEM = pltpu.SMEM
HBM = pltpu.HBM
DMA = pltpu.SemaphoreType.DMA

AXES = ("y", "x", "zh", "zl", "c")
SIZES = (4, 4, 4, 2, 2)
NY, NX, ZH, ZL, NC = SIZES
PEERS = ("y", "x", "zl", "c")
GROUP = NY * NX * ZL * NC


def shift(value, axis, step):
    n = lax.axis_size(axis)
    return lax.ppermute(value, axis, [(i, (i + step) % n) for i in range(n)])


def iota(shape, dim):
    return lax.broadcasted_iota(jnp.int32, shape, dim)


def one_hot(mask, dtype=jnp.bfloat16):
    return jnp.where(mask, 1.0, 0.0).astype(dtype)


def dot(a, b, dims=((1,), (0,))):
    return lax.dot_general(a, b, (dims, ((), ())), preferred_element_type=jnp.float32)


def shape(*dims, dtype=jnp.float32):
    return jax.ShapeDtypeStruct(dims, dtype)


def call(kernel, outs, spaces, args, scratch=(), flops=0):
    return pl.pallas_call(
        kernel,
        out_shape=outs,
        in_specs=[pl.BlockSpec(memory_space=s) for s in spaces],
        out_specs=jax.tree.map(lambda _: pl.BlockSpec(memory_space=VMEM), outs),
        scratch_shapes=list(scratch),
        cost_estimate=pl.CostEstimate(flops=flops, transcendentals=0, bytes_accessed=1 << 20),
        compiler_params=pltpu.CompilerParams(vmem_limit_bytes=40 << 20),
    )(*args)


def ranks(owner, owners):
    rows = owner.shape[1]
    before = one_hot(iota((LANES, LANES), 0) < iota((LANES, LANES), 1))
    ones = jnp.ones((LANES, LANES), jnp.bfloat16)
    seen = jnp.zeros((owners, LANES), jnp.float32)
    out = []
    for b in range(rows // LANES):
        mask = iota((owners, LANES), 0) == owner[:, b * LANES : (b + 1) * LANES]
        hot = one_hot(mask)
        prefix = dot(hot, before) + seen
        seen = seen + dot(hot, ones)
        out.append(jnp.sum(jnp.where(mask, prefix, 0.0), axis=0, keepdims=True))
    return jnp.concatenate(out, axis=1).astype(jnp.int32)


def pack_kernel(most, owned, kinds, index_hbm, cluster_hbm, child_hbm, pool_hbm, out, ints, pool, select, int_sems, pool_sem):
    fetch = pltpu.make_async_copy(pool_hbm, pool, pool_sem)
    small = [
        pltpu.make_async_copy(src, ints.at[k], int_sems.at[k])
        for k, src in enumerate((cluster_hbm, index_hbm, child_hbm))
    ]
    for copy in small:
        copy.start()
    fetch.start()
    for copy in small:
        copy.wait()
    rows, width = pool.shape
    blocks = width // LANES
    cluster = ints[0]
    owner = lax.div(cluster, owned)
    rank = ranks(owner, GROUP * ZH)
    quarter = lax.rem(owner, NY)
    dev = lax.div(owner, NY)
    core = lax.rem(dev, NC)
    z = lax.rem(lax.div(dev, NC), ZH * ZL)
    x = lax.div(dev, NC * ZH * ZL)
    peer = ((quarter * NX + x) * ZL + lax.rem(z, ZL)) * NC + core
    chunk = ZH * most
    slot = peer * chunk + lax.div(z, ZL) * most + rank
    label = lax.div(z, ZL) * (owned * kinds) + lax.rem(cluster, owned) * kinds + ints[2] + 1
    label = jnp.broadcast_to(label.astype(jnp.float32), (8, rows)).astype(jnp.bfloat16)
    index = (lax.rem(ints[1], rows) + 1).astype(jnp.float32)
    per = LANES // chunk
    lane = iota((LANES, per * LANES), 1)
    spread = one_hot(iota((LANES, per * LANES), 0) == lax.div(lane, LANES) * chunk + lax.rem(lane, chunk))
    for g in range(GROUP // per):
        mask = iota((LANES, rows), 0) == slot - g * LANES
        labels = dot(dot(label, one_hot(mask), ((1,), (1,))).astype(jnp.bfloat16), spread).astype(jnp.bfloat16)
        for p in range(per):
            out[g * per + p, blocks * chunk :, :] = labels[:, p * LANES : (p + 1) * LANES]
        source = jnp.sum(jnp.where(mask, index, 0.0), axis=1, keepdims=True).astype(jnp.int32) - 1
        select[g * LANES : (g + 1) * LANES, :] = one_hot(iota((LANES, rows), 1) == source)
    fetch.wait()
    step = 4 * LANES
    for g in range(0, GROUP * chunk, step):
        got = dot(select[g : g + step, :], pool[...]).astype(jnp.bfloat16)
        for p in range(step // chunk):
            for b in range(blocks):
                out[g // chunk + p, b * chunk : (b + 1) * chunk, :] = got[
                    p * chunk : (p + 1) * chunk, b * LANES : (b + 1) * LANES
                ]


def sum_kernel(chunk, order, where, old_hbm, came_hbm, *rest):
    outs, (came, old, total, sems, old_sem) = rest[:-5], rest[-5:]
    part, width = old.shape
    blocks = width // LANES
    per = LANES // chunk
    many = came.shape[0] // sems.shape[0]
    fetch = pltpu.make_async_copy(old_hbm.at[pl.ds(pl.multiple_of(where[0] * part, part), part), :], old, old_sem)
    copies = [
        pltpu.make_async_copy(came_hbm.at[pl.ds(k * many, many)], came.at[pl.ds(k * many, many)], sems.at[k])
        for k in range(sems.shape[0])
    ]
    for copy in copies:
        copy.start()
    fetch.start()
    segments = ZH * part
    row = iota((segments, LANES), 0) + 1
    place = lax.div(iota((segments, LANES), 1), chunk)
    ones = jnp.ones((2 * LANES, LANES), jnp.bfloat16)
    sums = jnp.zeros((segments, width), jnp.float32)
    count = jnp.zeros((segments, LANES), jnp.float32)
    for k, copy in enumerate(copies):
        copy.wait()
        for g in range(k * many, (k + 1) * many, 2 * per):
            hots = []
            for h in range(g, g + 2 * per, per):
                label = jnp.zeros((segments, LANES), jnp.float32)
                for p in range(per):
                    line = came[h + p, blocks * chunk :, :].astype(jnp.float32)[0:1]
                    label = jnp.where(place == p, line, label)
                hots.append(one_hot(row == label.astype(jnp.int32)))
            hot = jnp.concatenate(hots, axis=1)
            data = jnp.concatenate(
                [
                    jnp.concatenate([came[h, b * chunk : (b + 1) * chunk, :] for h in range(g, g + 2 * per)], axis=0)
                    for b in range(blocks)
                ],
                axis=1,
            )
            sums = sums + dot(hot, data)
            count = count + dot(hot, ones)
    total[:, :width] = sums
    total[:, width:] = count
    fetch.wait()
    own = pl.ds(pl.multiple_of(where[1] * part, part), part)
    total[own, :width] = total[own, :width] + old[...]
    for step, out in zip(order, outs):
        out[...] = total[pl.ds(pl.multiple_of(lax.rem(where[1] + step, ZH) * part, part), part), :]


def finish_kernel(*refs):
    ins, out = refs[:-1], refs[-1]
    width = out.shape[1] - LANES
    total = ins[0][...]
    for r in ins[1:]:
        total = total + r[...]
    count = total[:, width:]
    divisor = jnp.concatenate([count + 1.0] * (width // LANES), axis=1)
    out[:, :width] = total[:, :width] / divisor
    out[:, width:] = count


def place_kernel(order, where, *rest):
    ins, (fresh_ref, count_ref) = rest[:-2], rest[-2:]
    y = where[0]
    part, width = ins[0].shape[0], fresh_ref.shape[1]
    kinds = count_ref.shape[1]
    pick = iota((part, LANES), 1) == lax.rem(iota((part, LANES), 0), kinds)
    for dy, r in zip(order, ins):
        q = lax.rem(y - dy + NY, NY)
        fresh_ref[pl.ds(pl.multiple_of(q * part, part), part), :] = r[:, :width]
        count = jnp.where(pick, r[:, width:], 0.0)
        for k in range(part // kinds):
            line = jnp.sum(count[k * kinds : (k + 1) * kinds], axis=0, keepdims=True)
            count_ref[pl.ds(q * (part // kinds) + k, 1), :] = line[:, :kinds].astype(jnp.int32)


def per_device(pool_rows, sample_index, cluster_id, child_id, old_centroids):
    rows, width = pool_rows.shape
    block, kinds = old_centroids.shape[:2]
    owned = block // NY
    most = 4 * rows // (block * NX * ZH * ZL * NC)
    chunk = ZH * most
    part = owned * kinds
    wide = width + LANES
    long = chunk * (width // LANES) + 8
    where = jnp.stack([lax.axis_index("y"), lax.axis_index("zh")])

    lines = [a.reshape(1, rows) for a in (sample_index, cluster_id, child_id)]
    packed = call(
        functools.partial(pack_kernel, most, owned, kinds),
        shape(GROUP, long, LANES, dtype=jnp.bfloat16),
        [HBM] * 4,
        [*lines, pool_rows],
        [
            VMEM((3, 1, rows), jnp.int32),
            VMEM((rows, width), jnp.bfloat16),
            VMEM((GROUP * chunk, rows), jnp.bfloat16),
            DMA((3,)),
            DMA,
        ],
    )
    came = lax.all_to_all(packed, PEERS, split_axis=0, concat_axis=0, tiled=True)
    turns = [0, 1, 3, 2]
    pieces = call(
        functools.partial(sum_kernel, chunk, turns),
        [shape(part, wide)] * ZH,
        [SMEM, HBM, HBM],
        [where, old_centroids.reshape(block * kinds, width), came],
        [
            VMEM((GROUP, long, LANES), jnp.bfloat16),
            VMEM((part, width), jnp.float32),
            VMEM((ZH * part, wide), jnp.float32),
            DMA((4,)),
            DMA,
        ],
    )
    pieces = [pieces[0]] + [shift(p, "zh", t) for t, p in zip(turns[1:], pieces[1:])]
    fresh = call(finish_kernel, shape(part, wide), [VMEM] * ZH, pieces)
    quarters = [fresh] + [shift(fresh, "y", t) for t in turns[1:]]
    centroids, counts = call(
        functools.partial(place_kernel, turns),
        [shape(block * kinds, width), shape(block, kinds, dtype=jnp.int32)],
        [SMEM] + [VMEM] * NY,
        [where, *quarters],
    )
    return centroids.reshape(block, kinds, width), counts


def solution(mesh):
    fine = Mesh(mesh.devices.reshape(SIZES), AXES)
    dev = ("x", "zh", "zl", "c")
    placed = (
        P(AXES, None),
        P(AXES),
        P(AXES),
        P(AXES),
        P(dev, None, None),
    )
    return jax.shard_map(
        per_device,
        mesh=fine,
        in_specs=placed,
        out_specs=(P(dev, None, None), P(dev, None)),
        check_vma=False,
    )
```

```python
import functools

import jax
import jax.numpy as jnp
from jax import lax
from jax.experimental import pallas as pl
from jax.experimental.pallas import tpu as pltpu
from jax.sharding import Mesh, PartitionSpec as P


AXES = ("y", "x", "zh", "zl", "c")
SIZES = (4, 4, 4, 2, 2)
N, ZH, ZL, NC = 4, 4, 2, 2
NZ = ZH * ZL
CHUNKS = N * ZL
LANES = 128
TILE = 8
LOW = 32
VMEM = pltpu.VMEM
SMEM = pltpu.SMEM
HBM = pltpu.HBM
DMA = pltpu.SemaphoreType.DMA

RAW = [(2, 1), (2, 0), (1, 1), (3, 1), (1, 0), (3, 0), (0, 1)]
TURNS = [0, 1, 3, 2]


def permute(value, move):
    pairs = []
    for y in range(N):
        for x in range(N):
            for z in range(NZ):
                for c in range(NC):
                    ty, tx, tz, tc = move(y, x, z, c)
                    to = (((ty % N) * N + tx % N) * NZ + tz % NZ) * NC + tc % NC
                    pairs.append((((y * N + x) * NZ + z) * NC + c, to))
    return lax.ppermute(value, AXES, pairs)


def raw_move(step, swap):
    def move(y, x, z, c):
        if swap:
            z = z ^ 1 if c == 0 else (z + 1 if z % 2 else z - 1)
        return (y, x + step, z, c) if c == 0 else (y + step, x, z, c)

    return move


def cross_move(step):
    return lambda y, x, z, c: (y + step, x, z, c) if c == 0 else (y, x + step, z, c)


def iota(shape, dim):
    return lax.broadcasted_iota(jnp.int32, shape, dim)


def one_hot(mask, dtype=jnp.bfloat16):
    return jnp.where(mask, 1.0, 0.0).astype(dtype)


def dot(a, b, dims=((1,), (0,))):
    return lax.dot_general(a, b, (dims, ((), ())), preferred_element_type=jnp.float32)


def shape(*dims, dtype=jnp.float32):
    return jax.ShapeDtypeStruct(dims, dtype)


def call(kernel, outs, spaces, args, scratch=()):
    return pl.pallas_call(
        kernel,
        out_shape=outs,
        in_specs=[pl.BlockSpec(memory_space=s) for s in spaces],
        out_specs=jax.tree.map(lambda _: pl.BlockSpec(memory_space=VMEM), outs),
        scratch_shapes=list(scratch),
        compiler_params=pltpu.CompilerParams(vmem_limit_bytes=44 << 20),
    )(*args)


def ranks(hot, mask):
    owners, rows = hot.shape
    before = one_hot(iota((LANES, LANES), 0) < iota((LANES, LANES), 1))
    ones = jnp.ones((LANES, LANES), jnp.bfloat16)
    seen = jnp.zeros((owners, LANES), jnp.float32)
    out = []
    for b in range(rows // LANES):
        at = slice(b * LANES, (b + 1) * LANES)
        prefix = dot(hot[:, at], before) + seen
        seen = seen + dot(hot[:, at], ones)
        out.append(jnp.sum(jnp.where(mask[:, at], prefix, 0.0), axis=0, keepdims=True))
    return jnp.concatenate(out, axis=1).astype(jnp.int32)


def lines_of(where, most, owned, kinds, ints):
    a_me, b_me, odd, core = where[0], where[1], where[2], where[4]
    rows = ints.shape[2]
    index, cluster, child = ints[0], ints[1], ints[2]
    owner = lax.div(cluster, owned)
    quarter = lax.rem(owner, N)
    dev = lax.div(owner, N)
    to_core = lax.rem(dev, NC)
    z = lax.rem(lax.div(dev, NC), NZ)
    x = lax.div(dev, NC * NZ)
    a = x + (quarter - x) * core
    b = quarter + (x - quarter) * core
    step = lax.rem(a - a_me + N, N)
    swap = lax.rem(lax.rem(z, ZL) + odd, ZL)
    spot = ((step * ZL + swap) * N + b) * (ZH * NC) + lax.div(z, ZL) * NC + to_core
    spots = N * N * NZ * NC
    mask = iota((spots, rows), 0) == spot
    hot = one_hot(mask)
    rank = iota((most, rows), 0) == ranks(hot, mask)
    index = lax.rem(index, rows) + 1
    label = lax.rem(cluster, owned) * kinds + child + 1

    def spread(line):
        line = jnp.where(rank, line.astype(jnp.float32), 0.0)
        return dot(hot, line.astype(jnp.bfloat16), ((1,), (1,)))

    high = lax.div(index, LOW)
    source = spread(index - high * LOW) + spread(high * LOW)
    source = jnp.broadcast_to(source[:, None, :], (spots, most, most)).reshape(spots * most, most)
    pick = iota((spots * most, most), 1) == lax.rem(iota((spots * most, most), 0), most)
    source = jnp.sum(jnp.where(pick, source, 0.0), axis=1, keepdims=True).astype(jnp.int32)
    per = LANES // most
    tile = one_hot(iota((most, LANES), 0) == lax.rem(iota((most, LANES), 1), most))
    label = dot(spread(label).astype(jnp.bfloat16), tile)
    keep = lax.div(iota((spots, LANES), 1), most) == lax.rem(iota((spots, LANES), 0), per)
    label = jnp.sum(jnp.where(keep, label, 0.0).reshape(spots // per, per, LANES), axis=1)
    return source, label


def pack_kernel(most, owned, kinds, where, own_ref, came_ref, own_pool, came_pool, *rest):
    outs, (pool, select, sems) = rest[:CHUNKS], rest[CHUNKS:]
    rows, width = pool.shape[1:]
    columns = pl.ds(pl.multiple_of(where[4] * width, width), width)
    copies = [
        pltpu.make_async_copy(src.at[:, columns], pool.at[k], sems.at[k]) for k, src in enumerate((own_pool, came_pool))
    ]
    for copy in copies:
        copy.start()
    blocks = width // LANES
    slots = N * N * NZ * NC * most
    chunk = slots // CHUNKS
    labels = []
    for k, ints in enumerate((own_ref, came_ref)):
        source, label = lines_of(where, most, owned, kinds, ints)
        labels.append(label)
        group = 2 * chunk
        for g in range(0, slots, group):
            select[k, g : g + group, :] = one_hot(iota((group, rows), 1) + 1 == source[g : g + group])
    for k, copy in enumerate(copies):
        copy.wait()
        for g in range(0, slots, group):
            got = dot(select[k, g : g + group, :], pool[k]).astype(jnp.bfloat16)
            for j in range(group // chunk):
                for b in range(blocks):
                    at = (b * NC + k) * chunk
                    outs[g // chunk + j][at : at + chunk, :] = got[
                        j * chunk : (j + 1) * chunk, b * LANES : (b + 1) * LANES
                    ]
    lines = chunk // LANES
    line = iota((TILE, LANES), 0)
    for j in range(CHUNKS):
        tile = jnp.zeros((TILE, LANES), jnp.float32)
        for k in range(NC):
            for h in range(lines):
                tile = jnp.where(line == k * lines + h, labels[k][j * lines + h : j * lines + h + 1], tile)
        outs[j][blocks * NC * chunk :, :] = tile.astype(jnp.bfloat16)


def sum_kernel(most, kinds2, where, *rest):
    ins, outs, (total, tally) = rest[:CHUNKS], rest[CHUNKS:-2], rest[-2:]
    width = total.shape[1]
    blocks = width // LANES
    chunk = (ins[0].shape[0] - TILE) // (blocks * NC)
    lines = chunk // LANES
    segments = LANES // most * kinds2
    row = iota((segments, LANES), 0)
    base = lax.div(iota((1, LANES), 1), most) * kinds2 - 1
    ones = jnp.ones((TILE, 2 * NC * LANES), jnp.bfloat16)
    part = total.shape[0] // N
    for h in range(lines):
        sums = jnp.zeros((segments, width), jnp.float32)
        count = jnp.zeros((TILE, segments), jnp.float32)
        for j in range(0, CHUNKS, 2):
            hots, data = [], []
            for r in ins[j : j + 2]:
                labels = r[blocks * NC * chunk :, :].astype(jnp.float32).astype(jnp.int32)
                for k in range(NC):
                    label = labels[k * lines + h : k * lines + h + 1]
                    hots.append(one_hot(row == jnp.where(label > 0, base + label, -1)))
                    at = [(b * NC + k) * chunk + h * LANES for b in range(blocks)]
                    data.append(jnp.concatenate([r[i : i + LANES, :] for i in at], axis=1))
            hot = jnp.concatenate(hots, axis=1)
            sums = sums + dot(hot, jnp.concatenate(data, axis=0))
            count = count + dot(ones, hot, ((1,), (1,)))
        total[h * segments : (h + 1) * segments, :] = sums
        for k in range(segments // part):
            tally[h * (segments // part) + k] = count[:, k * part : (k + 1) * part]
    for step, out in zip(TURNS, outs):
        b = lax.rem(where[1] + step, N)
        for k in range(blocks):
            out[k * part : (k + 1) * part, :] = total[
                pl.ds(pl.multiple_of(b * part, part), part), k * LANES : (k + 1) * LANES
            ]
        out[blocks * part :, :] = tally[b]


def cross_kernel(where, *rest):
    ins, outs, total = rest[:N], rest[N:-1], rest[-1]
    total[...] = (ins[0][...] + ins[1][...]) + (ins[2][...] + ins[3][...])
    part = outs[0].shape[0] - TILE
    blocks = (total.shape[0] - TILE) // LANES
    some = part // blocks
    for step, out in zip(TURNS, outs):
        at = pl.multiple_of(lax.rem(where[3] + step, ZH) * some, some)
        for k in range(blocks):
            out[k * some : (k + 1) * some, :] = total[pl.ds(k * LANES + at, some), :]
        out[part:, :] = total[blocks * LANES :, :]


def depth_kernel(blocks, where, *rest):
    ins, (other_ref, mine_ref, total) = rest[:ZH], rest[ZH:]
    total[...] = (ins[0][...] + ins[1][...]) + (ins[2][...] + ins[3][...])
    part = other_ref.shape[0]
    some = part // blocks
    for out, core in ((other_ref, 1 - where[4]), (mine_ref, where[4])):
        for k in range(blocks):
            at = pl.multiple_of(k * NC * some + core * some, some)
            out[k * some : (k + 1) * some, :] = total[pl.ds(at, some), :]
    mine_ref[part:, :] = total[NC * part :, :]


def finish_kernel(kinds, where, old_ref, mine_ref, came_ref, out, sums):
    half = came_ref.shape[0]
    core = where[4]
    sums[pl.ds(pl.multiple_of(core * half, half), half), :] = mine_ref[:half, :]
    sums[pl.ds(pl.multiple_of((1 - core) * half, half), half), :] = came_ref[...]
    blocks = old_ref.shape[1] // LANES
    part = 2 * half // blocks
    lane = iota((part, LANES), 1)
    here = lane == iota((part, LANES), 0) + (where[3] * NC + core) * part
    count = jnp.sum(jnp.where(here, mine_ref[half : half + 1, :], 0.0), axis=1, keepdims=True)
    divisor = jnp.broadcast_to(count + 1.0, (part, LANES))
    rows = pl.ds(pl.multiple_of(where[5] * part, part), part)
    for k in range(blocks):
        at = slice(k * part, (k + 1) * part)
        out[at, :] = (sums[at, :] + old_ref[rows, k * LANES : (k + 1) * LANES]) / divisor
    count = jnp.where(lane == lax.rem(iota((part, LANES), 0), kinds), count, 0.0)
    line = iota((TILE, LANES), 0)
    tile = jnp.zeros((TILE, LANES), jnp.float32)
    for k in range(part // kinds):
        tile = jnp.where(line == k, jnp.sum(count[k * kinds : (k + 1) * kinds], axis=0, keepdims=True), tile)
    out[blocks * part :, :] = tile


def place_kernel(where, *rest):
    ins, (fresh_ref, count_ref) = rest[:-2], rest[-2:]
    blocks = fresh_ref.shape[1] // LANES
    part = (ins[0].shape[0] - TILE) // blocks
    kinds = count_ref.shape[1]
    for step, r in zip(TURNS, ins):
        q = lax.rem(where[5] - step + N, N)
        rows = pl.ds(pl.multiple_of(q * part, part), part)
        for k in range(blocks):
            fresh_ref[rows, k * LANES : (k + 1) * LANES] = r[k * part : (k + 1) * part, :]
        for k in range(part // kinds):
            count_ref[pl.ds(q * (part // kinds) + k, 1), :] = r[blocks * part + k : blocks * part + k + 1, :kinds].astype(
                jnp.int32
            )


def per_device(pool_rows, sample_index, cluster_id, child_id, old_centroids):
    rows, width = pool_rows.shape
    block, kinds = old_centroids.shape[:2]
    owned = block // N
    most = 4 * rows // (block * N * NZ * NC)
    half = width // NC
    blocks = half // LANES
    chunk = N * NZ * NC * N * most // CHUNKS
    part = owned * kinds
    y, x, zh, zl, c = (lax.axis_index(a) for a in AXES)
    where = jnp.stack([x + (y - x) * c, y + (x - y) * c, zl, zh, c, y])

    def other_core(y, x, z, c):
        return y, x, z, 1 - c

    ints = jnp.stack([sample_index, cluster_id, child_id]).reshape(3, 1, rows)
    packed = call(
        functools.partial(pack_kernel, most, owned, kinds),
        [shape(blocks * NC * chunk + TILE, LANES, dtype=jnp.bfloat16)] * CHUNKS,
        [SMEM, VMEM, VMEM, HBM, HBM],
        [where, ints, permute(ints, other_core), pool_rows, permute(pool_rows, other_core)],
        [VMEM((NC, rows, half), jnp.bfloat16), VMEM((NC, CHUNKS * chunk, rows), jnp.bfloat16), DMA((NC,))],
    )
    came = [packed[0]] + [permute(packed[step * ZL + swap], raw_move(step, swap)) for step, swap in RAW]
    segments = N * ZH * NC * part
    pieces = call(
        functools.partial(sum_kernel, most, part),
        [shape(blocks * segments // N + TILE, LANES)] * N,
        [SMEM] + [VMEM] * CHUNKS,
        [where, *came],
        [VMEM((segments, half), jnp.float32), VMEM((N, TILE, LANES), jnp.float32)],
    )
    pieces = [pieces[0]] + [permute(p, cross_move(t)) for t, p in zip(TURNS[1:], pieces[1:])]
    pieces = call(
        cross_kernel,
        [shape(blocks * NC * part + TILE, LANES)] * ZH,
        [SMEM] + [VMEM] * N,
        [where, *pieces],
        [VMEM((blocks * segments // N + TILE, LANES), jnp.float32)],
    )
    pieces = [pieces[0]] + [
        permute(p, lambda y, x, z, c, t=t: (y, x, z + ZL * t, c)) for t, p in zip(TURNS[1:], pieces[1:])
    ]
    other, mine = call(
        functools.partial(depth_kernel, blocks),
        [shape(blocks * part, LANES), shape(blocks * part + TILE, LANES)],
        [SMEM] + [VMEM] * ZH,
        [where, *pieces],
        [VMEM((blocks * NC * part + TILE, LANES), jnp.float32)],
    )
    fresh = call(
        functools.partial(finish_kernel, kinds),
        shape(NC * blocks * part + TILE, LANES),
        [SMEM, VMEM, VMEM, VMEM],
        [where, old_centroids.reshape(block * kinds, width), mine, permute(other, other_core)],
        [VMEM((NC * blocks * part, LANES), jnp.float32)],
    )
    quarters = [fresh] + [permute(fresh, lambda y, x, z, c, t=t: (y + t, x, z, c)) for t in TURNS[1:]]
    centroids, counts = call(
        place_kernel,
        [shape(block * kinds, width), shape(block, kinds, dtype=jnp.int32)],
        [SMEM] + [VMEM] * N,
        [where, *quarters],
    )
    return centroids.reshape(block, kinds, width), counts


def solution(mesh):
    fine = Mesh(mesh.devices.reshape(SIZES), AXES)
    dev = ("x", "zh", "zl", "c")
    placed = (P(AXES, None), P(AXES), P(AXES), P(AXES), P(dev, None, None))
    return jax.shard_map(
        per_device,
        mesh=fine,
        in_specs=placed,
        out_specs=(P(dev, None, None), P(dev, None)),
        check_vma=False,
    )
```

```python
import functools

import jax
import jax.numpy as jnp
from jax import lax
from jax.experimental import pallas as pl
from jax.experimental.pallas import tpu as pltpu
from jax.sharding import Mesh, PartitionSpec as P


AXES = ("y", "x", "zh", "zl", "c")
SIZES = (4, 4, 4, 2, 2)
N, ZH, ZL, NC = 4, 4, 2, 2
NZ = ZH * ZL
CHUNKS = N * ZL
LANES = 128
TILE = 8
LOW = 32
VMEM = pltpu.VMEM
SMEM = pltpu.SMEM
HBM = pltpu.HBM
DMA = pltpu.SemaphoreType.DMA

RAW = [(2, 1), (2, 0), (0, 1), (1, 1), (3, 1), (1, 0), (3, 0)]
FIRST = 3
TURNS = [0, 1, 3, 2]
EARLY = 4


def permute(value, move):
    pairs = []
    for y in range(N):
        for x in range(N):
            for z in range(NZ):
                for c in range(NC):
                    ty, tx, tz, tc = move(y, x, z, c)
                    to = (((ty % N) * N + tx % N) * NZ + tz % NZ) * NC + tc % NC
                    pairs.append((((y * N + x) * NZ + z) * NC + c, to))
    return lax.ppermute(value, AXES, pairs)


def raw_move(step, swap):
    def move(y, x, z, c):
        if swap:
            z = z ^ 1 if c == 0 else (z + 1 if z % 2 else z - 1)
        return (y, x + step, z, c) if c == 0 else (y + step, x, z, c)

    return move


def cross_move(step):
    return lambda y, x, z, c: (y + step, x, z, c) if c == 0 else (y, x + step, z, c)


def iota(shape, dim):
    return lax.broadcasted_iota(jnp.int32, shape, dim)


def one_hot(mask, dtype=jnp.bfloat16):
    return jnp.where(mask, 1.0, 0.0).astype(dtype)


def dot(a, b, dims=((1,), (0,))):
    return lax.dot_general(a, b, (dims, ((), ())), preferred_element_type=jnp.float32)


def shape(*dims, dtype=jnp.float32):
    return jax.ShapeDtypeStruct(dims, dtype)


def call(kernel, outs, spaces, args, scratch=()):
    return pl.pallas_call(
        kernel,
        out_shape=outs,
        in_specs=[pl.BlockSpec(memory_space=s) for s in spaces],
        out_specs=jax.tree.map(lambda _: pl.BlockSpec(memory_space=VMEM), outs),
        scratch_shapes=list(scratch),
        compiler_params=pltpu.CompilerParams(vmem_limit_bytes=44 << 20),
    )(*args)


def ranks(hot, mask):
    owners, rows = hot.shape
    before = one_hot(iota((LANES, LANES), 0) < iota((LANES, LANES), 1))
    ones = jnp.ones((LANES, LANES), jnp.bfloat16)
    seen = jnp.zeros((owners, LANES), jnp.float32)
    out = []
    for b in range(rows // LANES):
        at = slice(b * LANES, (b + 1) * LANES)
        prefix = dot(hot[:, at], before) + seen
        seen = seen + dot(hot[:, at], ones)
        out.append(jnp.sum(jnp.where(mask[:, at], prefix, 0.0), axis=0, keepdims=True))
    return jnp.concatenate(out, axis=1).astype(jnp.int32)


def lines_of(where, most, owned, kinds, ints):
    a_me, b_me, odd, core = where[0], where[1], where[2], where[4]
    rows = ints.shape[2]
    index, cluster, child = ints[0], ints[1], ints[2]
    owner = lax.div(cluster, owned)
    quarter = lax.rem(owner, N)
    dev = lax.div(owner, N)
    to_core = lax.rem(dev, NC)
    z = lax.rem(lax.div(dev, NC), NZ)
    x = lax.div(dev, NC * NZ)
    a = x + (quarter - x) * core
    b = quarter + (x - quarter) * core
    step = lax.rem(a - a_me + N, N)
    swap = lax.rem(lax.rem(z, ZL) + odd, ZL)
    spot = ((step * ZL + swap) * N + b) * (ZH * NC) + lax.div(z, ZL) * NC + to_core
    spots = N * N * NZ * NC
    mask = iota((spots, rows), 0) == spot
    hot = one_hot(mask)
    rank = iota((most, rows), 0) == ranks(hot, mask)
    index = lax.rem(index, rows) + 1
    label = lax.rem(cluster, owned) * kinds + child + 1

    def spread(line):
        line = jnp.where(rank, line.astype(jnp.float32), 0.0)
        return dot(hot, line.astype(jnp.bfloat16), ((1,), (1,)))

    high = lax.div(index, LOW)
    source = spread(index - high * LOW) + spread(high * LOW)
    per = LANES // most
    tile = one_hot(iota((most, LANES), 0) == lax.rem(iota((most, LANES), 1), most))
    label = dot(spread(label).astype(jnp.bfloat16), tile)
    keep = lax.div(iota((spots, LANES), 1), most) == lax.rem(iota((spots, LANES), 0), per)
    label = jnp.sum(jnp.where(keep, label, 0.0).reshape(spots // per, per, LANES), axis=1)
    return source, label


def lines_kernel(most, owned, kinds, where, ints_ref, source_ref, label_ref):
    source_ref[...], label_ref[...] = lines_of(where, most, owned, kinds, ints_ref)


def own_kernel(most, owned, kinds, where, ints_ref, pool_hbm, source_ref, label_ref, pool, sem):
    width = pool.shape[1]
    columns = pl.ds(pl.multiple_of(where[4] * width, width), width)
    copy = pltpu.make_async_copy(pool_hbm.at[:, columns], pool, sem)
    copy.start()
    source_ref[...], label_ref[...] = lines_of(where, most, owned, kinds, ints_ref)
    copy.wait()


def fill_kernel(chunks, where, own_source, own_label, came_source, came_label, own_pool, came_pool, *rest):
    outs, select = rest[:-1], rest[-1]
    rows, width = own_pool.shape
    blocks = width // LANES
    most = own_source.shape[1]
    spots = own_source.shape[0] // CHUNKS
    chunk = spots * most
    pick = iota((chunk, most), 1) == lax.rem(iota((chunk, most), 0), most)
    lines = chunk // LANES
    line = iota((TILE, LANES), 0)
    for i, j in enumerate(chunks):
        tile = jnp.zeros((TILE, LANES), jnp.float32)
        for k, (source_ref, label_ref) in enumerate(((own_source, own_label), (came_source, came_label))):
            source = source_ref[j * spots : (j + 1) * spots, :]
            source = jnp.broadcast_to(source[:, None, :], (spots, most, most)).reshape(chunk, most)
            source = jnp.sum(jnp.where(pick, source, 0.0), axis=1, keepdims=True).astype(jnp.int32)
            select[k, i * chunk : (i + 1) * chunk, :] = one_hot(iota((chunk, rows), 1) + 1 == source)
            for h in range(lines):
                tile = jnp.where(line == k * lines + h, label_ref[j * lines + h : j * lines + h + 1, :], tile)
        outs[i][blocks * NC * chunk :, :] = tile.astype(jnp.bfloat16)
    columns = pl.ds(pl.multiple_of(where[4] * width, width), width)
    for k in range(NC):
        pool = came_pool[:, columns] if k else own_pool[...]
        for g in range(0, len(chunks), 2):
            some = min(2, len(chunks) - g)
            got = dot(select[k, g * chunk : (g + some) * chunk, :], pool).astype(jnp.bfloat16)
            for i in range(some):
                for b in range(blocks):
                    at = (b * NC + k) * chunk
                    outs[g + i][at : at + chunk, :] = got[i * chunk : (i + 1) * chunk, b * LANES : (b + 1) * LANES]


def add_up(most, kinds2, ins, total, tally, before=None):
    width = total.shape[1]
    blocks = width // LANES
    chunk = (ins[0].shape[0] - TILE) // (blocks * NC)
    lines = chunk // LANES
    segments = LANES // most * kinds2
    row = iota((segments, LANES), 0)
    base = lax.div(iota((1, LANES), 1), most) * kinds2 - 1
    ones = jnp.ones((TILE, 2 * NC * LANES), jnp.bfloat16)
    per = segments // LANES
    for h in range(lines):
        at = slice(h * segments, (h + 1) * segments)
        sums = jnp.zeros((segments, width), jnp.float32) if before is None else before[0][at, :]
        count = jnp.zeros((TILE, segments), jnp.float32)
        for j in range(0, len(ins), 2):
            hots, data = [], []
            for r in ins[j : j + 2]:
                labels = r[blocks * NC * chunk :, :].astype(jnp.float32).astype(jnp.int32)
                for k in range(NC):
                    label = labels[k * lines + h : k * lines + h + 1]
                    hots.append(one_hot(row == jnp.where(label > 0, base + label, -1)))
                    first = [(b * NC + k) * chunk + h * LANES for b in range(blocks)]
                    data.append(jnp.concatenate([r[i : i + LANES, :] for i in first], axis=1))
            hot = jnp.concatenate(hots, axis=1)
            sums = sums + dot(hot, jnp.concatenate(data, axis=0))
            count = count + dot(ones, hot, ((1,), (1,)))
        total[at, :] = sums
        for k in range(per):
            line = count[:, k * LANES : (k + 1) * LANES]
            tally[h * per + k] = line if before is None else line + before[1][h * per + k]


def early_kernel(most, kinds2, *rest):
    ins, (total, tally) = rest[:-2], rest[-2:]
    add_up(most, kinds2, ins, total, tally)


def late_kernel(most, kinds2, where, sum_ref, tally_ref, *rest):
    outs, (total, tally) = rest[-N - 2 : -2], rest[-2:]
    add_up(most, kinds2, rest[: -N - 2], total, tally, (sum_ref, tally_ref))
    blocks = total.shape[1] // LANES
    part = total.shape[0] // N
    for step, out in zip(TURNS, outs):
        b = lax.rem(where[1] + step, N)
        for k in range(blocks):
            out[k * part : (k + 1) * part, :] = total[
                pl.ds(pl.multiple_of(b * part, part), part), k * LANES : (k + 1) * LANES
            ]
        out[blocks * part :, :] = tally[b]


def cross_kernel(where, *rest):
    ins, outs, total = rest[:N], rest[N:-1], rest[-1]
    total[...] = (ins[0][...] + ins[1][...]) + (ins[2][...] + ins[3][...])
    part = outs[0].shape[0] - TILE
    blocks = (total.shape[0] - TILE) // LANES
    some = part // blocks
    for step, out in zip(TURNS, outs):
        at = pl.multiple_of(lax.rem(where[3] + step, ZH) * some, some)
        for k in range(blocks):
            out[k * some : (k + 1) * some, :] = total[pl.ds(k * LANES + at, some), :]
        out[part:, :] = total[blocks * LANES :, :]


def depth_kernel(blocks, where, *rest):
    ins, (other_ref, mine_ref, total) = rest[:ZH], rest[ZH:]
    total[...] = (ins[0][...] + ins[1][...]) + (ins[2][...] + ins[3][...])
    part = other_ref.shape[0]
    some = part // blocks
    for out, core in ((other_ref, 1 - where[4]), (mine_ref, where[4])):
        for k in range(blocks):
            at = pl.multiple_of(k * NC * some + core * some, some)
            out[k * some : (k + 1) * some, :] = total[pl.ds(at, some), :]
    mine_ref[part:, :] = total[NC * part :, :]


def finish_kernel(kinds, where, old_ref, mine_ref, came_ref, out, sums):
    half = came_ref.shape[0]
    core = where[4]
    sums[pl.ds(pl.multiple_of(core * half, half), half), :] = mine_ref[:half, :]
    sums[pl.ds(pl.multiple_of((1 - core) * half, half), half), :] = came_ref[...]
    blocks = old_ref.shape[1] // LANES
    part = 2 * half // blocks
    lane = iota((part, LANES), 1)
    here = lane == iota((part, LANES), 0) + (where[3] * NC + core) * part
    count = jnp.sum(jnp.where(here, mine_ref[half : half + 1, :], 0.0), axis=1, keepdims=True)
    divisor = jnp.broadcast_to(count + 1.0, (part, LANES))
    rows = pl.ds(pl.multiple_of(where[5] * part, part), part)
    for k in range(blocks):
        at = slice(k * part, (k + 1) * part)
        out[at, :] = (sums[at, :] + old_ref[rows, k * LANES : (k + 1) * LANES]) / divisor
    count = jnp.where(lane == lax.rem(iota((part, LANES), 0), kinds), count, 0.0)
    line = iota((TILE, LANES), 0)
    tile = jnp.zeros((TILE, LANES), jnp.float32)
    for k in range(part // kinds):
        tile = jnp.where(line == k, jnp.sum(count[k * kinds : (k + 1) * kinds], axis=0, keepdims=True), tile)
    out[blocks * part :, :] = tile


def place_kernel(where, *rest):
    ins, (fresh_ref, count_ref) = rest[:-2], rest[-2:]
    blocks = fresh_ref.shape[1] // LANES
    part = (ins[0].shape[0] - TILE) // blocks
    kinds = count_ref.shape[1]
    for step, r in zip(TURNS, ins):
        q = lax.rem(where[5] - step + N, N)
        rows = pl.ds(pl.multiple_of(q * part, part), part)
        for k in range(blocks):
            fresh_ref[rows, k * LANES : (k + 1) * LANES] = r[k * part : (k + 1) * part, :]
        for k in range(part // kinds):
            count_ref[pl.ds(q * (part // kinds) + k, 1), :] = r[blocks * part + k : blocks * part + k + 1, :kinds].astype(
                jnp.int32
            )


def per_device(pool_rows, sample_index, cluster_id, child_id, old_centroids):
    rows, width = pool_rows.shape
    block, kinds = old_centroids.shape[:2]
    owned = block // N
    most = 4 * rows // (block * N * NZ * NC)
    half = width // NC
    blocks = half // LANES
    chunk = N * NZ * NC * N * most // CHUNKS
    part = owned * kinds
    y, x, zh, zl, c = (lax.axis_index(a) for a in AXES)
    where = jnp.stack([x + (y - x) * c, y + (x - y) * c, zl, zh, c, y])

    def other_core(y, x, z, c):
        return y, x, z, 1 - c

    came_pool = permute(pool_rows, other_core)
    ints = jnp.stack([sample_index, cluster_id, child_id]).reshape(3, 1, rows)
    came_ints = permute(ints, other_core)
    slots = CHUNKS * chunk
    lines = [shape(slots // most, most), shape(slots // LANES, LANES)]
    *own_lines, own_pool = call(
        functools.partial(own_kernel, most, owned, kinds),
        [*lines, shape(rows, half, dtype=jnp.bfloat16)],
        [SMEM, VMEM, HBM],
        [where, ints, pltpu.with_memory_space_constraint(pool_rows, HBM)],
        [DMA],
    )
    came_lines = call(functools.partial(lines_kernel, most, owned, kinds), lines, [SMEM, VMEM], [where, came_ints])
    came = []
    for moves in (RAW[:FIRST], RAW[FIRST:] + [(0, 0)]):
        packed = call(
            functools.partial(fill_kernel, [step * ZL + swap for step, swap in moves]),
            [shape(blocks * NC * chunk + TILE, LANES, dtype=jnp.bfloat16)] * len(moves),
            [SMEM] + [VMEM] * 6,
            [where, *own_lines, *came_lines, own_pool, came_pool],
            [VMEM((NC, len(moves) * chunk, rows), jnp.bfloat16)],
        )
        came += [permute(p, raw_move(*move)) if any(move) else p for p, move in zip(packed, moves)]
    segments = N * ZH * NC * part
    sums = [shape(segments, half), shape(segments // LANES, TILE, LANES)]
    early = call(functools.partial(early_kernel, most, part), sums, [VMEM] * EARLY, came[:EARLY])
    pieces = call(
        functools.partial(late_kernel, most, part),
        [shape(blocks * segments // N + TILE, LANES)] * N,
        [SMEM] + [VMEM] * (2 + CHUNKS - EARLY),
        [where, *early, *came[EARLY:]],
        [VMEM(a.shape, jnp.float32) for a in sums],
    )
    pieces = [pieces[0]] + [permute(p, cross_move(t)) for t, p in zip(TURNS[1:], pieces[1:])]
    pieces = call(
        cross_kernel,
        [shape(blocks * NC * part + TILE, LANES)] * ZH,
        [SMEM] + [VMEM] * N,
        [where, *pieces],
        [VMEM((blocks * segments // N + TILE, LANES), jnp.float32)],
    )
    pieces = [pieces[0]] + [
        permute(p, lambda y, x, z, c, t=t: (y, x, z + ZL * t, c)) for t, p in zip(TURNS[1:], pieces[1:])
    ]
    other, mine = call(
        functools.partial(depth_kernel, blocks),
        [shape(blocks * part, LANES), shape(blocks * part + TILE, LANES)],
        [SMEM] + [VMEM] * ZH,
        [where, *pieces],
        [VMEM((blocks * NC * part + TILE, LANES), jnp.float32)],
    )
    fresh = call(
        functools.partial(finish_kernel, kinds),
        shape(NC * blocks * part + TILE, LANES),
        [SMEM, VMEM, VMEM, VMEM],
        [where, old_centroids.reshape(block * kinds, width), mine, permute(other, other_core)],
        [VMEM((NC * blocks * part, LANES), jnp.float32)],
    )
    quarters = [fresh] + [permute(fresh, lambda y, x, z, c, t=t: (y + t, x, z, c)) for t in TURNS[1:]]
    centroids, counts = call(
        place_kernel,
        [shape(block * kinds, width), shape(block, kinds, dtype=jnp.int32)],
        [SMEM] + [VMEM] * N,
        [where, *quarters],
    )
    return centroids.reshape(block, kinds, width), counts


def solution(mesh):
    fine = Mesh(mesh.devices.reshape(SIZES), AXES)
    dev = ("x", "zh", "zl", "c")
    placed = (P(AXES, None), P(AXES), P(AXES), P(AXES), P(dev, None, None))
    return jax.shard_map(
        per_device,
        mesh=fine,
        in_specs=placed,
        out_specs=(P(dev, None, None), P(dev, None)),
        check_vma=False,
    )
```

```python
import functools

import jax
import jax.numpy as jnp
from jax import lax
from jax.experimental import pallas as pl
from jax.experimental.pallas import tpu as pltpu
from jax.sharding import Mesh, PartitionSpec as P


AXES = ("y", "x", "zh", "zl", "c")
SIZES = (4, 4, 4, 2, 2)
N, ZH, ZL, NC = 4, 4, 2, 2
NZ = ZH * ZL
CHUNKS = N * ZL
LANES = 128
TILE = 8
LOW = 32
VMEM = pltpu.VMEM
SMEM = pltpu.SMEM
HBM = pltpu.HBM
DMA = pltpu.SemaphoreType.DMA

RAW = [(2, 1), (2, 0), (0, 1), (1, 1), (3, 0), (3, 1), (1, 0)]
FIRST = 3
DEEP = [0, 2, 1, 3]
TURNS = [0, 1, 3, 2]
EARLY = 4


def permute(value, move):
    pairs = []
    for y in range(N):
        for x in range(N):
            for z in range(NZ):
                for c in range(NC):
                    ty, tx, tz, tc = move(y, x, z, c)
                    to = (((ty % N) * N + tx % N) * NZ + tz % NZ) * NC + tc % NC
                    pairs.append((((y * N + x) * NZ + z) * NC + c, to))
    return lax.ppermute(value, AXES, pairs)


def raw_move(step, swap):
    def move(y, x, z, c):
        if swap:
            z = z ^ 1 if c == 0 else (z + 1 if z % 2 else z - 1)
        return (y, x + step, z, c) if c == 0 else (y + step, x, z, c)

    return move


def cross_move(step):
    return lambda y, x, z, c: (y + step, x, z, c) if c == 0 else (y, x + step, z, c)


def iota(shape, dim):
    return lax.broadcasted_iota(jnp.int32, shape, dim)


def one_hot(mask, dtype=jnp.bfloat16):
    return jnp.where(mask, 1.0, 0.0).astype(dtype)


def dot(a, b, dims=((1,), (0,))):
    return lax.dot_general(a, b, (dims, ((), ())), preferred_element_type=jnp.float32)


def shape(*dims, dtype=jnp.float32):
    return jax.ShapeDtypeStruct(dims, dtype)


def call(kernel, outs, spaces, args, scratch=()):
    return pl.pallas_call(
        kernel,
        out_shape=outs,
        in_specs=[pl.BlockSpec(memory_space=s) for s in spaces],
        out_specs=jax.tree.map(lambda _: pl.BlockSpec(memory_space=VMEM), outs),
        scratch_shapes=list(scratch),
        compiler_params=pltpu.CompilerParams(vmem_limit_bytes=44 << 20),
    )(*args)


def ranks(hot, mask):
    owners, rows = hot.shape
    wide = (LANES, 2 * LANES)
    before = one_hot((iota(wide, 0) < iota(wide, 1)) | (iota(wide, 1) >= LANES))
    seen = jnp.zeros((owners, LANES), jnp.float32)
    out = []
    for b in range(rows // LANES):
        at = slice(b * LANES, (b + 1) * LANES)
        counted = dot(hot[:, at], before)
        out.append(jnp.sum(jnp.where(mask[:, at], counted[:, :LANES] + seen, 0.0), axis=0, keepdims=True))
        seen = seen + counted[:, LANES:]
    return jnp.concatenate(out, axis=1).astype(jnp.int32)


def lines_of(where, most, owned, kinds, ints):
    a_me, b_me, odd, z_me, core = where[0], where[1], where[2], where[3], where[4]
    rows = ints.shape[2]
    index, cluster, child = ints[0], ints[1], ints[2]
    owner = lax.div(cluster, owned)
    quarter = lax.rem(owner, N)
    dev = lax.div(owner, N)
    to_core = lax.rem(dev, NC)
    z = lax.rem(lax.div(dev, NC), NZ)
    x = lax.div(dev, NC * NZ)
    a = x + (quarter - x) * core
    b = quarter + (x - quarter) * core
    step = lax.rem(a - a_me + N, N)
    swap = lax.rem(lax.rem(z, ZL) + odd, ZL)
    b = lax.rem(b - b_me + N, N)
    pair = lax.rem(lax.div(z, ZL) - z_me + swap * core * (1 - 2 * odd) + 2 * ZH, ZH)
    spot = ((step * ZL + swap) * N + b) * (ZH * NC) + pair * NC + lax.rem(to_core + core, NC)
    spots = N * N * NZ * NC
    mask = iota((spots, rows), 0) == spot
    hot = one_hot(mask)
    rank = iota((most, rows), 0) == ranks(hot, mask)
    index = lax.rem(index, rows) + 1
    label = lax.rem(cluster, owned) * kinds + child + 1

    high = lax.div(index, LOW)
    lines = [jnp.where(rank, a.astype(jnp.float32), 0.0) for a in (index - high * LOW, high * LOW, label)]
    spread = dot(hot, jnp.concatenate(lines, axis=0).astype(jnp.bfloat16), ((1,), (1,)))
    source = spread[:, :most] + spread[:, most : 2 * most]
    per = LANES // most
    tile = one_hot(iota((most, LANES), 0) == lax.rem(iota((most, LANES), 1), most))
    label = dot(spread[:, 2 * most :].astype(jnp.bfloat16), tile)
    keep = lax.div(iota((spots, LANES), 1), most) == lax.rem(iota((spots, LANES), 0), per)
    label = jnp.sum(jnp.where(keep, label, 0.0).reshape(spots // per, per, LANES), axis=1)
    return source, label


def lines_kernel(most, owned, kinds, where, ints_ref, source_ref, label_ref):
    source_ref[...], label_ref[...] = lines_of(where, most, owned, kinds, ints_ref)


def pool_kernel(most, owned, kinds, where, ints_ref, pool_hbm, source_ref, label_ref, pool, sem):
    width = pool.shape[1]
    columns = pl.ds(pl.multiple_of(where[4] * width, width), width)
    copy = pltpu.make_async_copy(pool_hbm.at[:, columns], pool, sem)
    copy.start()
    source_ref[...], label_ref[...] = lines_of(where, most, owned, kinds, ints_ref)
    copy.wait()


def fill_kernel(chunks, where, own_source, own_label, came_source, came_label, own_pool, came_pool, *rest):
    outs, select = rest[:-1], rest[-1]
    rows, width = own_pool.shape
    blocks = width // LANES
    most = own_source.shape[1]
    spots = own_source.shape[0] // CHUNKS
    chunk = spots * most
    pick = iota((chunk, most), 1) == lax.rem(iota((chunk, most), 0), most)
    lines = chunk // LANES
    line = iota((TILE, LANES), 0)
    for i, j in enumerate(chunks):
        tile = jnp.zeros((TILE, LANES), jnp.float32)
        for k, (source_ref, label_ref) in enumerate(((own_source, own_label), (came_source, came_label))):
            source = source_ref[j * spots : (j + 1) * spots, :]
            source = jnp.broadcast_to(source[:, None, :], (spots, most, most)).reshape(chunk, most)
            source = jnp.sum(jnp.where(pick, source, 0.0), axis=1, keepdims=True).astype(jnp.int32)
            select[k, i * chunk : (i + 1) * chunk, :] = one_hot(iota((chunk, rows), 1) + 1 == source)
            for h in range(lines):
                tile = jnp.where(line == k * lines + h, label_ref[j * lines + h : j * lines + h + 1, :], tile)
        outs[i][blocks * NC * chunk :, :] = tile.astype(jnp.bfloat16)
    columns = pl.ds(pl.multiple_of(where[4] * width, width), width)
    for k in range(NC):
        pool = came_pool[:, columns] if k else own_pool[...]
        for g in range(0, len(chunks), 2):
            some = min(2, len(chunks) - g)
            got = dot(select[k, g * chunk : (g + some) * chunk, :], pool).astype(jnp.bfloat16)
            for i in range(some):
                for b in range(blocks):
                    at = (b * NC + k) * chunk
                    outs[g + i][at : at + chunk, :] = got[i * chunk : (i + 1) * chunk, b * LANES : (b + 1) * LANES]


def add_up(most, kinds2, ins, h, before=None):
    chunk = N * ZH * NC * most
    blocks = (ins[0].shape[0] - TILE) // (NC * chunk)
    lines = chunk // LANES
    segments = LANES // most * kinds2
    row = iota((segments, LANES), 0)
    base = lax.div(iota((1, LANES), 1), most) * kinds2 - 1
    ones = jnp.ones((TILE, 2 * NC * LANES), jnp.bfloat16)
    sums, count = before if before is not None else (0.0, 0.0)
    for j in range(0, len(ins), 2):
        hots, data = [], []
        for r in ins[j : j + 2]:
            labels = r[blocks * NC * chunk :, :].astype(jnp.float32).astype(jnp.int32)
            for k in range(NC):
                label = labels[k * lines + h : k * lines + h + 1]
                hots.append(one_hot(row == jnp.where(label > 0, base + label, -1)))
                first = [(b * NC + k) * chunk + h * LANES for b in range(blocks)]
                data.append(jnp.concatenate([r[i : i + LANES, :] for i in first], axis=1))
        hot = jnp.concatenate(hots, axis=1)
        sums = sums + dot(hot, jnp.concatenate(data, axis=0))
        count = count + dot(ones, hot, ((1,), (1,)))
    return sums, count


def early_kernel(most, kinds2, *rest):
    ins, (total, tally) = rest[:-2], rest[-2:]
    lines = tally.shape[0]
    segments = total.shape[0] // lines
    for h in range(lines):
        total[h * segments : (h + 1) * segments, :], tally[h] = add_up(most, kinds2, ins, h)


def late_kernel(most, kinds2, sum_ref, tally_ref, *rest):
    ins, outs = rest[:-N], rest[-N:]
    lines = tally_ref.shape[0]
    segments = sum_ref.shape[0] // lines
    blocks = sum_ref.shape[1] // LANES
    part = lines * segments // N
    for h in range(lines):
        before = (sum_ref[h * segments : (h + 1) * segments, :], tally_ref[h])
        sums, count = add_up(most, kinds2, ins, h, before)
        for p in range(segments // part):
            out = outs[TURNS.index(h * (segments // part) + p)]
            for k in range(blocks):
                out[k * part : (k + 1) * part, :] = sums[p * part : (p + 1) * part, k * LANES : (k + 1) * LANES]
            out[blocks * part :, :] = count[:, p * part : (p + 1) * part]


def cross_kernel(*rest):
    ins, outs = rest[:N], rest[N:]
    part = outs[0].shape[0] - TILE
    blocks = (ins[0].shape[0] - TILE) // LANES
    some = part // blocks
    total = (ins[0][...] + ins[1][...]) + (ins[2][...] + ins[3][...])
    for step, out in zip(DEEP, outs):
        for k in range(blocks):
            out[k * some : (k + 1) * some, :] = total[k * LANES + step * some : k * LANES + (step + 1) * some]
        tile = total[blocks * LANES :]
        out[part:, :] = jnp.concatenate([tile[:, step * some :], tile[:, : step * some]], axis=1) if step else tile


def depth_kernel(some, *rest):
    ins, (other_ref, mine_ref) = rest[:ZH], rest[ZH:]
    total = (ins[0][...] + ins[1][...]) + (ins[2][...] + ins[3][...])
    part = other_ref.shape[0]
    for side, out in enumerate((mine_ref, other_ref)):
        for k in range(part // some):
            at = (k * NC + side) * some
            out[k * some : (k + 1) * some, :] = total[at : at + some]
    mine_ref[part:, :] = total[NC * part :]


def finish_kernel(kinds, where, old_ref, mine_ref, came_ref, out, sums):
    half, width = came_ref.shape[0], old_ref.shape[1]
    core = where[4]
    sums[pl.ds(pl.multiple_of(core * half, half), half), :] = mine_ref[:half, :]
    sums[pl.ds(pl.multiple_of((1 - core) * half, half), half), :] = came_ref[...]
    blocks = width // LANES
    part = 2 * half // blocks
    lane = iota((part, LANES), 1)
    here = lane == iota((part, LANES), 0)
    count = jnp.sum(jnp.where(here, mine_ref[half : half + 1, :], 0.0), axis=1, keepdims=True)
    divisor = jnp.broadcast_to(count + 1.0, (part, LANES))
    rows = pl.ds(pl.multiple_of(where[5] * part, part), part)
    for k in range(blocks):
        at = slice(k * LANES, (k + 1) * LANES)
        out[:, at] = (sums[k * part : (k + 1) * part, :] + old_ref[rows, at]) / divisor
    count = jnp.where(lane == lax.rem(iota((part, LANES), 0), kinds), count, 0.0)
    line = iota((part, LANES), 0)
    tile = jnp.zeros((part, LANES), jnp.float32)
    for k in range(part // kinds):
        tile = jnp.where(line == k, jnp.sum(count[k * kinds : (k + 1) * kinds], axis=0, keepdims=True), tile)
    out[:, width:] = tile


def place_kernel(where, *rest):
    ins, (fresh_ref, count_ref) = rest[:-2], rest[-2:]
    part, width = ins[0].shape[0], fresh_ref.shape[1]
    kinds = count_ref.shape[1]
    for step, r in zip(TURNS, ins):
        q = lax.rem(where[5] - step + N, N)
        fresh_ref[pl.ds(pl.multiple_of(q * part, part), part), :] = r[:, :width]
        for k in range(part // kinds):
            line = r[k : k + 1, width : width + kinds]
            count_ref[pl.ds(q * (part // kinds) + k, 1), :] = line.astype(jnp.int32)


def per_device(pool_rows, sample_index, cluster_id, child_id, old_centroids):
    rows, width = pool_rows.shape
    block, kinds = old_centroids.shape[:2]
    owned = block // N
    most = 4 * rows // (block * N * NZ * NC)
    half = width // NC
    blocks = half // LANES
    chunk = N * NZ * NC * N * most // CHUNKS
    part = owned * kinds
    y, x, zh, zl, c = (lax.axis_index(a) for a in AXES)
    where = jnp.stack([x + (y - x) * c, y + (x - y) * c, zl, zh, c, y])

    def other_core(y, x, z, c):
        return y, x, z, 1 - c

    ints = jnp.stack([sample_index, cluster_id, child_id]).reshape(3, 1, rows)
    came_ints = permute(ints, other_core)
    came_pool = permute(pool_rows, other_core)
    slots = CHUNKS * chunk
    lines = [shape(slots // most, most), shape(slots // LANES, LANES)]
    own_lines = call(functools.partial(lines_kernel, most, owned, kinds), lines, [SMEM, VMEM], [where, ints])
    *came_lines, own_pool = call(
        functools.partial(pool_kernel, most, owned, kinds),
        [*lines, shape(rows, half, dtype=jnp.bfloat16)],
        [SMEM, VMEM, HBM],
        [where, came_ints, pltpu.with_memory_space_constraint(pool_rows, HBM)],
        [DMA],
    )
    came = []
    for moves in (RAW[:FIRST], RAW[FIRST:] + [(0, 0)]):
        packed = call(
            functools.partial(fill_kernel, [step * ZL + swap for step, swap in moves]),
            [shape(blocks * NC * chunk + TILE, LANES, dtype=jnp.bfloat16)] * len(moves),
            [SMEM] + [VMEM] * 6,
            [where, *own_lines, *came_lines, own_pool, came_pool],
            [VMEM((NC, len(moves) * chunk, rows), jnp.bfloat16)],
        )
        came += [permute(p, raw_move(*move)) if any(move) else p for p, move in zip(packed, moves)]
    segments = N * ZH * NC * part
    sums = [shape(segments, half), shape(chunk // LANES, TILE, segments * LANES // chunk)]
    early = call(functools.partial(early_kernel, most, part), sums, [VMEM] * EARLY, came[:EARLY])
    pieces = call(
        functools.partial(late_kernel, most, part),
        [shape(blocks * segments // N + TILE, LANES)] * N,
        [VMEM] * (2 + CHUNKS - EARLY),
        [*early, *came[EARLY:]],
    )
    pieces = [pieces[0]] + [permute(p, cross_move(t)) for t, p in zip(TURNS[1:], pieces[1:])]
    pieces = call(cross_kernel, [shape(blocks * NC * part + TILE, LANES)] * ZH, [VMEM] * N, pieces)
    pieces = [pieces[0]] + [
        permute(p, lambda y, x, z, c, t=t: (y, x, z + ZL * t, c)) for t, p in zip(DEEP[1:], pieces[1:])
    ]
    other, mine = call(
        functools.partial(depth_kernel, part),
        [shape(blocks * part, LANES), shape(blocks * part + TILE, LANES)],
        [VMEM] * ZH,
        pieces,
    )
    fresh = call(
        functools.partial(finish_kernel, kinds),
        shape(part, width + LANES),
        [SMEM, VMEM, VMEM, VMEM],
        [where, old_centroids.reshape(block * kinds, width), mine, permute(other, other_core)],
        [VMEM((NC * blocks * part, LANES), jnp.float32)],
    )
    quarters = [fresh] + [permute(fresh, lambda y, x, z, c, t=t: (y + t, x, z, c)) for t in TURNS[1:]]
    centroids, counts = call(
        place_kernel,
        [shape(block * kinds, width), shape(block, kinds, dtype=jnp.int32)],
        [SMEM] + [VMEM] * N,
        [where, *quarters],
    )
    return centroids.reshape(block, kinds, width), counts


def solution(mesh):
    fine = Mesh(mesh.devices.reshape(SIZES), AXES)
    dev = ("x", "zh", "zl", "c")
    placed = (P(AXES, None), P(AXES), P(AXES), P(AXES), P(dev, None, None))

    return jax.shard_map(
        per_device,
        mesh=fine,
        in_specs=placed,
        out_specs=(P(dev, None, None), P(dev, None)),
        check_vma=False,
    )
```

```python
import functools

import jax
import jax.numpy as jnp
from jax import lax
from jax.experimental import pallas as pl
from jax.experimental.pallas import tpu as pltpu
from jax.sharding import Mesh, PartitionSpec as P


AXES = ("y", "x", "zh", "zl", "c")
SIZES = (4, 4, 4, 2, 2)
N, ZH, ZL, NC = 4, 4, 2, 2
NZ = ZH * ZL
CHUNKS = N * ZL
LANES = 128
TILE = 8
LOW = 32
VMEM = pltpu.VMEM
SMEM = pltpu.SMEM
HBM = pltpu.HBM
DMA = pltpu.SemaphoreType.DMA

RAW = [(2, 1), (2, 0), (0, 1), (1, 1), (3, 0), (3, 1), (1, 0)]
FIRST = 3
CROSS = [0, 2, 1, 3]
DEEP = [0, 2, 1, 3]
TURNS = [0, 1, 3, 2]
EARLY = 4


def permute(value, move):
    pairs = []
    for y in range(N):
        for x in range(N):
            for z in range(NZ):
                for c in range(NC):
                    ty, tx, tz, tc = move(y, x, z, c)
                    to = (((ty % N) * N + tx % N) * NZ + tz % NZ) * NC + tc % NC
                    pairs.append((((y * N + x) * NZ + z) * NC + c, to))
    return lax.ppermute(value, AXES, pairs)


def raw_move(step, swap):
    def move(y, x, z, c):
        if swap:
            z = z ^ 1 if c == 0 else (z + 1 if z % 2 else z - 1)
        return (y, x + step, z, c) if c == 0 else (y + step, x, z, c)

    return move


def cross_move(step):
    return lambda y, x, z, c: (y + step, x, z, c) if c == 0 else (y, x + step, z, c)


def iota(shape, dim):
    return lax.broadcasted_iota(jnp.int32, shape, dim)


def one_hot(mask, dtype=jnp.bfloat16):
    return jnp.where(mask, 1.0, 0.0).astype(dtype)


def dot(a, b, dims=((1,), (0,))):
    return lax.dot_general(a, b, (dims, ((), ())), preferred_element_type=jnp.float32)


def shape(*dims, dtype=jnp.float32):
    return jax.ShapeDtypeStruct(dims, dtype)


def call(kernel, outs, spaces, args, scratch=()):
    return pl.pallas_call(
        kernel,
        out_shape=outs,
        in_specs=[pl.BlockSpec(memory_space=s) for s in spaces],
        out_specs=jax.tree.map(lambda _: pl.BlockSpec(memory_space=VMEM), outs),
        scratch_shapes=list(scratch),
        compiler_params=pltpu.CompilerParams(vmem_limit_bytes=44 << 20),
    )(*args)


def ranks(hot, mask):
    owners, rows = hot.shape
    wide = (LANES, 2 * LANES)
    before = one_hot((iota(wide, 0) < iota(wide, 1)) | (iota(wide, 1) >= LANES))
    seen = jnp.zeros((owners, LANES), jnp.float32)
    out = []
    for b in range(rows // LANES):
        at = slice(b * LANES, (b + 1) * LANES)
        counted = dot(hot[:, at], before)
        out.append(jnp.sum(jnp.where(mask[:, at], counted[:, :LANES] + seen, 0.0), axis=0, keepdims=True))
        seen = seen + counted[:, LANES:]
    return jnp.concatenate(out, axis=1).astype(jnp.int32)


def lines_of(where, most, owned, kinds, ints):
    a_me, b_me, odd, z_me, core = where[0], where[1], where[2], where[3], where[4]
    rows = ints.shape[2]
    index, cluster, child = ints[0], ints[1], ints[2]
    owner = lax.div(cluster, owned)
    quarter = lax.rem(owner, N)
    dev = lax.div(owner, N)
    to_core = lax.rem(dev, NC)
    z = lax.rem(lax.div(dev, NC), NZ)
    x = lax.div(dev, NC * NZ)
    a = x + (quarter - x) * core
    b = quarter + (x - quarter) * core
    step = lax.rem(a - a_me + N, N)
    swap = lax.rem(lax.rem(z, ZL) + odd, ZL)
    b = lax.rem(b - b_me + N, N)
    pair = lax.rem(lax.div(z, ZL) - z_me + swap * core * (1 - 2 * odd) + 2 * ZH, ZH)
    spot = ((step * ZL + swap) * N + b) * (ZH * NC) + pair * NC + lax.rem(to_core + core, NC)
    spots = N * N * NZ * NC
    mask = iota((spots, rows), 0) == spot
    hot = one_hot(mask)
    rank = iota((most, rows), 0) == ranks(hot, mask)
    index = lax.rem(index, rows) + 1
    label = lax.rem(cluster, owned) * kinds + child + 1

    high = lax.div(index, LOW)
    lines = [jnp.where(rank, a.astype(jnp.float32), 0.0) for a in (index - high * LOW, high * LOW, label)]
    spread = dot(hot, jnp.concatenate(lines, axis=0).astype(jnp.bfloat16), ((1,), (1,)))
    source = spread[:, :most] + spread[:, most : 2 * most]
    per = LANES // most
    tile = one_hot(iota((most, LANES), 0) == lax.rem(iota((most, LANES), 1), most))
    label = dot(spread[:, 2 * most :].astype(jnp.bfloat16), tile)
    keep = lax.div(iota((spots, LANES), 1), most) == lax.rem(iota((spots, LANES), 0), per)
    label = jnp.sum(jnp.where(keep, label, 0.0).reshape(spots // per, per, LANES), axis=1)
    return source, label


def lines_kernel(most, owned, kinds, where, ints_ref, source_ref, label_ref):
    source_ref[...], label_ref[...] = lines_of(where, most, owned, kinds, ints_ref)


def pool_kernel(most, owned, kinds, where, ints_ref, pool_hbm, source_ref, label_ref, pool, sem):
    width = pool.shape[1]
    columns = pl.ds(pl.multiple_of(where[4] * width, width), width)
    copy = pltpu.make_async_copy(pool_hbm.at[:, columns], pool, sem)
    copy.start()
    source_ref[...], label_ref[...] = lines_of(where, most, owned, kinds, ints_ref)
    copy.wait()


def fill_kernel(chunks, where, own_source, own_label, came_source, came_label, own_pool, came_pool, *rest):
    outs, select = rest[:-1], rest[-1]
    rows, width = own_pool.shape
    blocks = width // LANES
    most = own_source.shape[1]
    spots = own_source.shape[0] // CHUNKS
    chunk = spots * most
    pick = iota((chunk, most), 1) == lax.rem(iota((chunk, most), 0), most)
    lines = chunk // LANES
    line = iota((TILE, LANES), 0)
    for i, j in enumerate(chunks):
        tile = jnp.zeros((TILE, LANES), jnp.float32)
        for k, (source_ref, label_ref) in enumerate(((own_source, own_label), (came_source, came_label))):
            source = source_ref[j * spots : (j + 1) * spots, :]
            source = jnp.broadcast_to(source[:, None, :], (spots, most, most)).reshape(chunk, most)
            source = jnp.sum(jnp.where(pick, source, 0.0), axis=1, keepdims=True).astype(jnp.int32)
            select[k, i * chunk : (i + 1) * chunk, :] = one_hot(iota((chunk, rows), 1) + 1 == source)
            for h in range(lines):
                tile = jnp.where(line == k * lines + h, label_ref[j * lines + h : j * lines + h + 1, :], tile)
        outs[i][blocks * NC * chunk :, :] = tile.astype(jnp.bfloat16)
    columns = pl.ds(pl.multiple_of(where[4] * width, width), width)
    for k in range(NC):
        pool = came_pool[:, columns] if k else own_pool[...]
        for g in range(0, len(chunks), 2):
            some = min(2, len(chunks) - g)
            got = dot(select[k, g * chunk : (g + some) * chunk, :], pool).astype(jnp.bfloat16)
            for i in range(some):
                for b in range(blocks):
                    at = (b * NC + k) * chunk
                    outs[g + i][at : at + chunk, :] = got[i * chunk : (i + 1) * chunk, b * LANES : (b + 1) * LANES]


def add_up(most, kinds2, ins, h, before=None):
    chunk = N * ZH * NC * most
    blocks = (ins[0].shape[0] - TILE) // (NC * chunk)
    lines = chunk // LANES
    segments = LANES // most * kinds2
    row = iota((segments, LANES), 0)
    base = lax.div(iota((1, LANES), 1), most) * kinds2 - 1
    ones = jnp.ones((TILE, 2 * NC * LANES), jnp.bfloat16)
    sums, count = before if before is not None else (0.0, 0.0)
    for j in range(0, len(ins), 2):
        hots, data = [], []
        for r in ins[j : j + 2]:
            labels = r[blocks * NC * chunk :, :].astype(jnp.float32).astype(jnp.int32)
            for k in range(NC):
                label = labels[k * lines + h : k * lines + h + 1]
                hots.append(one_hot(row == jnp.where(label > 0, base + label, -1)))
                first = [(b * NC + k) * chunk + h * LANES for b in range(blocks)]
                data.append(jnp.concatenate([r[i : i + LANES, :] for i in first], axis=1))
        hot = jnp.concatenate(hots, axis=1)
        sums = sums + dot(hot, jnp.concatenate(data, axis=0))
        count = count + dot(ones, hot, ((1,), (1,)))
    return sums, count


def early_kernel(most, kinds2, *rest):
    ins, (total, tally) = rest[:-2], rest[-2:]
    lines = tally.shape[0]
    segments = total.shape[0] // lines
    for h in range(lines):
        total[h * segments : (h + 1) * segments, :], tally[h] = add_up(most, kinds2, ins, h)


def late_kernel(most, kinds2, sum_ref, tally_ref, *rest):
    ins, outs = rest[:-N], rest[-N:]
    lines = tally_ref.shape[0]
    segments = sum_ref.shape[0] // lines
    blocks = sum_ref.shape[1] // LANES
    part = lines * segments // N
    for h in range(lines):
        before = (sum_ref[h * segments : (h + 1) * segments, :], tally_ref[h])
        sums, count = add_up(most, kinds2, ins, h, before)
        for p in range(segments // part):
            out = outs[CROSS.index(h * (segments // part) + p)]
            for k in range(blocks):
                out[k * part : (k + 1) * part, :] = sums[p * part : (p + 1) * part, k * LANES : (k + 1) * LANES]
            out[blocks * part :, :] = count[:, p * part : (p + 1) * part]


def cross_kernel(*rest):
    ins, outs = rest[:N], rest[N:]
    part = outs[0].shape[0] - TILE
    blocks = (ins[0].shape[0] - TILE) // LANES
    some = part // blocks
    total = (ins[0][...] + ins[1][...]) + (ins[2][...] + ins[3][...])
    for step, out in zip(DEEP, outs):
        for k in range(blocks):
            out[k * some : (k + 1) * some, :] = total[k * LANES + step * some : k * LANES + (step + 1) * some]
        tile = total[blocks * LANES :]
        out[part:, :] = jnp.concatenate([tile[:, step * some :], tile[:, : step * some]], axis=1) if step else tile


def depth_kernel(some, *rest):
    ins, (other_ref, mine_ref) = rest[:ZH], rest[ZH:]
    total = (ins[0][...] + ins[1][...]) + (ins[2][...] + ins[3][...])
    part = other_ref.shape[0]
    for side, out in enumerate((mine_ref, other_ref)):
        for k in range(part // some):
            at = (k * NC + side) * some
            out[k * some : (k + 1) * some, :] = total[at : at + some]
    mine_ref[part:, :] = total[NC * part :]


def finish_kernel(kinds, where, old_ref, mine_ref, came_ref, out, sums):
    half, width = came_ref.shape[0], old_ref.shape[1]
    core = where[4]
    sums[pl.ds(pl.multiple_of(core * half, half), half), :] = mine_ref[:half, :]
    sums[pl.ds(pl.multiple_of((1 - core) * half, half), half), :] = came_ref[...]
    blocks = width // LANES
    part = 2 * half // blocks
    lane = iota((part, LANES), 1)
    here = lane == iota((part, LANES), 0)
    count = jnp.sum(jnp.where(here, mine_ref[half : half + 1, :], 0.0), axis=1, keepdims=True)
    divisor = jnp.broadcast_to(count + 1.0, (part, LANES))
    rows = pl.ds(pl.multiple_of(where[5] * part, part), part)
    for k in range(blocks):
        at = slice(k * LANES, (k + 1) * LANES)
        out[:, at] = (sums[k * part : (k + 1) * part, :] + old_ref[rows, at]) / divisor
    count = jnp.where(lane == lax.rem(iota((part, LANES), 0), kinds), count, 0.0)
    line = iota((part, LANES), 0)
    tile = jnp.zeros((part, LANES), jnp.float32)
    for k in range(part // kinds):
        tile = jnp.where(line == k, jnp.sum(count[k * kinds : (k + 1) * kinds], axis=0, keepdims=True), tile)
    out[:, width:] = tile


def place_kernel(where, *rest):
    ins, (fresh_ref, count_ref) = rest[:-2], rest[-2:]
    part, width = ins[0].shape[0], fresh_ref.shape[1]
    kinds = count_ref.shape[1]
    for step, r in zip(TURNS, ins):
        q = lax.rem(where[5] - step + N, N)
        fresh_ref[pl.ds(pl.multiple_of(q * part, part), part), :] = r[:, :width]
        for k in range(part // kinds):
            line = r[k : k + 1, width : width + kinds]
            count_ref[pl.ds(q * (part // kinds) + k, 1), :] = line.astype(jnp.int32)


def per_device(pool_rows, sample_index, cluster_id, child_id, old_centroids):
    rows, width = pool_rows.shape
    block, kinds = old_centroids.shape[:2]
    owned = block // N
    most = 4 * rows // (block * N * NZ * NC)
    half = width // NC
    blocks = half // LANES
    chunk = N * NZ * NC * N * most // CHUNKS
    part = owned * kinds
    y, x, zh, zl, c = (lax.axis_index(a) for a in AXES)
    where = jnp.stack([x + (y - x) * c, y + (x - y) * c, zl, zh, c, y])

    def other_core(y, x, z, c):
        return y, x, z, 1 - c

    ints = jnp.stack([sample_index, cluster_id, child_id]).reshape(3, 1, rows)
    came_ints = permute(ints, other_core)
    came_pool = permute(pool_rows, other_core)
    slots = CHUNKS * chunk
    lines = [shape(slots // most, most), shape(slots // LANES, LANES)]
    own_lines = call(functools.partial(lines_kernel, most, owned, kinds), lines, [SMEM, VMEM], [where, ints])
    *came_lines, own_pool = call(
        functools.partial(pool_kernel, most, owned, kinds),
        [*lines, shape(rows, half, dtype=jnp.bfloat16)],
        [SMEM, VMEM, HBM],
        [where, came_ints, pltpu.with_memory_space_constraint(pool_rows, HBM)],
        [DMA],
    )
    came = []
    for moves in (RAW[:FIRST], RAW[FIRST:] + [(0, 0)]):
        packed = call(
            functools.partial(fill_kernel, [step * ZL + swap for step, swap in moves]),
            [shape(blocks * NC * chunk + TILE, LANES, dtype=jnp.bfloat16)] * len(moves),
            [SMEM] + [VMEM] * 6,
            [where, *own_lines, *came_lines, own_pool, came_pool],
            [VMEM((NC, len(moves) * chunk, rows), jnp.bfloat16)],
        )
        came += [permute(p, raw_move(*move)) if any(move) else p for p, move in zip(packed, moves)]
    segments = N * ZH * NC * part
    sums = [shape(segments, half), shape(chunk // LANES, TILE, segments * LANES // chunk)]
    early = call(functools.partial(early_kernel, most, part), sums, [VMEM] * EARLY, came[:EARLY])
    pieces = call(
        functools.partial(late_kernel, most, part),
        [shape(blocks * segments // N + TILE, LANES)] * N,
        [VMEM] * (2 + CHUNKS - EARLY),
        [*early, *came[EARLY:]],
    )
    pieces = [pieces[0]] + [permute(p, cross_move(t)) for t, p in zip(CROSS[1:], pieces[1:])]
    pieces = call(cross_kernel, [shape(blocks * NC * part + TILE, LANES)] * ZH, [VMEM] * N, pieces)
    pieces = [pieces[0]] + [
        permute(p, lambda y, x, z, c, t=t: (y, x, z + ZL * t, c)) for t, p in zip(DEEP[1:], pieces[1:])
    ]
    other, mine = call(
        functools.partial(depth_kernel, part),
        [shape(blocks * part, LANES), shape(blocks * part + TILE, LANES)],
        [VMEM] * ZH,
        pieces,
    )
    fresh = call(
        functools.partial(finish_kernel, kinds),
        shape(part, width + LANES),
        [SMEM, VMEM, VMEM, VMEM],
        [where, old_centroids.reshape(block * kinds, width), mine, permute(other, other_core)],
        [VMEM((NC * blocks * part, LANES), jnp.float32)],
    )
    quarters = [fresh] + [permute(fresh, lambda y, x, z, c, t=t: (y + t, x, z, c)) for t in TURNS[1:]]
    centroids, counts = call(
        place_kernel,
        [shape(block * kinds, width), shape(block, kinds, dtype=jnp.int32)],
        [SMEM] + [VMEM] * N,
        [where, *quarters],
    )
    return centroids.reshape(block, kinds, width), counts


def solution(mesh):
    fine = Mesh(mesh.devices.reshape(SIZES), AXES)
    dev = ("x", "zh", "zl", "c")
    placed = (P(AXES, None), P(AXES), P(AXES), P(AXES), P(dev, None, None))

    return jax.shard_map(
        per_device,
        mesh=fine,
        in_specs=placed,
        out_specs=(P(dev, None, None), P(dev, None)),
        check_vma=False,
    )
```

```python
import functools

import jax
import jax.numpy as jnp
from jax import lax
from jax.experimental import pallas as pl
from jax.experimental.pallas import tpu as pltpu
from jax.sharding import Mesh, PartitionSpec as P


AXES = ("y", "x", "zh", "zl", "c")
SIZES = (4, 4, 4, 2, 2)
N, ZH, ZL, NC = 4, 4, 2, 2
NZ = ZH * ZL
CHUNKS = N * ZL
LANES = 128
TILE = 8
LOW = 32
VMEM = pltpu.VMEM
SMEM = pltpu.SMEM
HBM = pltpu.HBM
DMA = pltpu.SemaphoreType.DMA

RAW = [(2, 1), (2, 0), (0, 1), (1, 1), (3, 0), (3, 1), (1, 0)]
FIRST = 3
CROSS = [0, 2, 1, 3]
DEEP = [0, 2, 1, 3]
TURNS = [0, 2, 1, 3]
EARLY = 4


def permute(value, move):
    pairs = []
    for y in range(N):
        for x in range(N):
            for z in range(NZ):
                for c in range(NC):
                    ty, tx, tz, tc = move(y, x, z, c)
                    to = (((ty % N) * N + tx % N) * NZ + tz % NZ) * NC + tc % NC
                    pairs.append((((y * N + x) * NZ + z) * NC + c, to))
    return lax.ppermute(value, AXES, pairs)


def raw_move(step, swap):
    def move(y, x, z, c):
        if swap:
            z = z ^ 1 if c == 0 else (z + 1 if z % 2 else z - 1)
        return (y, x + step, z, c) if c == 0 else (y + step, x, z, c)

    return move


def cross_move(step):
    return lambda y, x, z, c: (y + step, x, z, c) if c == 0 else (y, x + step, z, c)


def iota(shape, dim):
    return lax.broadcasted_iota(jnp.int32, shape, dim)


def one_hot(mask, dtype=jnp.bfloat16):
    return jnp.where(mask, 1.0, 0.0).astype(dtype)


def dot(a, b, dims=((1,), (0,))):
    return lax.dot_general(a, b, (dims, ((), ())), preferred_element_type=jnp.float32)


def shape(*dims, dtype=jnp.float32):
    return jax.ShapeDtypeStruct(dims, dtype)


def call(kernel, outs, spaces, args, scratch=()):
    return pl.pallas_call(
        kernel,
        out_shape=outs,
        in_specs=[pl.BlockSpec(memory_space=s) for s in spaces],
        out_specs=jax.tree.map(lambda _: pl.BlockSpec(memory_space=VMEM), outs),
        scratch_shapes=list(scratch),
        compiler_params=pltpu.CompilerParams(vmem_limit_bytes=44 << 20),
    )(*args)


def ranks(hot, mask):
    owners, rows = hot.shape
    wide = (LANES, 2 * LANES)
    before = one_hot((iota(wide, 0) < iota(wide, 1)) | (iota(wide, 1) >= LANES))
    seen = jnp.zeros((owners, LANES), jnp.float32)
    out = []
    for b in range(rows // LANES):
        at = slice(b * LANES, (b + 1) * LANES)
        counted = dot(hot[:, at], before)
        out.append(jnp.sum(jnp.where(mask[:, at], counted[:, :LANES] + seen, 0.0), axis=0, keepdims=True))
        seen = seen + counted[:, LANES:]
    return jnp.concatenate(out, axis=1).astype(jnp.int32)


def lines_of(where, most, owned, kinds, ints):
    a_me, b_me, odd, z_me, core = where[0], where[1], where[2], where[3], where[4]
    rows = ints.shape[2]
    index, cluster, child = ints[0], ints[1], ints[2]
    owner = lax.div(cluster, owned)
    quarter = lax.rem(owner, N)
    dev = lax.div(owner, N)
    to_core = lax.rem(dev, NC)
    z = lax.rem(lax.div(dev, NC), NZ)
    x = lax.div(dev, NC * NZ)
    a = x + (quarter - x) * core
    b = quarter + (x - quarter) * core
    step = lax.rem(a - a_me + N, N)
    swap = lax.rem(lax.rem(z, ZL) + odd, ZL)
    b = lax.rem(b - b_me + N, N)
    pair = lax.rem(lax.div(z, ZL) - z_me + swap * core * (1 - 2 * odd) + 2 * ZH, ZH)
    spot = ((step * ZL + swap) * N + b) * (ZH * NC) + pair * NC + lax.rem(to_core + core, NC)
    spots = N * N * NZ * NC
    mask = iota((spots, rows), 0) == spot
    hot = one_hot(mask)
    rank = iota((most, rows), 0) == ranks(hot, mask)
    index = lax.rem(index, rows) + 1
    label = lax.rem(cluster, owned) * kinds + child + 1

    high = lax.div(index, LOW)
    lines = [jnp.where(rank, a.astype(jnp.float32), 0.0) for a in (index - high * LOW, high * LOW, label)]
    spread = dot(hot, jnp.concatenate(lines, axis=0).astype(jnp.bfloat16), ((1,), (1,)))
    source = spread[:, :most] + spread[:, most : 2 * most]
    per = LANES // most
    tile = one_hot(iota((most, LANES), 0) == lax.rem(iota((most, LANES), 1), most))
    label = dot(spread[:, 2 * most :].astype(jnp.bfloat16), tile)
    keep = lax.div(iota((spots, LANES), 1), most) == lax.rem(iota((spots, LANES), 0), per)
    label = jnp.sum(jnp.where(keep, label, 0.0).reshape(spots // per, per, LANES), axis=1)
    return source, label


def lines_kernel(most, owned, kinds, where, ints_ref, source_ref, label_ref):
    source_ref[...], label_ref[...] = lines_of(where, most, owned, kinds, ints_ref)


def pool_kernel(most, owned, kinds, where, ints_ref, pool_hbm, source_ref, label_ref, pool, sem):
    copy = pltpu.make_async_copy(pool_hbm, pool, sem)
    copy.start()
    source_ref[...], label_ref[...] = lines_of(where, most, owned, kinds, ints_ref)
    copy.wait()


def fill_kernel(chunks, where, own_source, own_label, came_source, came_label, own_pool, came_pool, *rest):
    outs, select = rest[:-1], rest[-1]
    rows, width = own_pool.shape[0], own_pool.shape[1] // NC
    blocks = width // LANES
    most = own_source.shape[1]
    spots = own_source.shape[0] // CHUNKS
    chunk = spots * most
    pick = iota((chunk, most), 1) == lax.rem(iota((chunk, most), 0), most)
    lines = chunk // LANES
    line = iota((TILE, LANES), 0)
    for i, j in enumerate(chunks):
        tile = jnp.zeros((TILE, LANES), jnp.float32)
        for k, (source_ref, label_ref) in enumerate(((own_source, own_label), (came_source, came_label))):
            source = source_ref[j * spots : (j + 1) * spots, :]
            source = jnp.broadcast_to(source[:, None, :], (spots, most, most)).reshape(chunk, most)
            source = jnp.sum(jnp.where(pick, source, 0.0), axis=1, keepdims=True).astype(jnp.int32)
            select[k, i * chunk : (i + 1) * chunk, :] = one_hot(iota((chunk, rows), 1) + 1 == source)
            for h in range(lines):
                tile = jnp.where(line == k * lines + h, label_ref[j * lines + h : j * lines + h + 1, :], tile)
        outs[i][blocks * NC * chunk :, :] = tile.astype(jnp.bfloat16)
    columns = pl.ds(pl.multiple_of(where[4] * width, width), width)
    for k in range(NC):
        pool = (came_pool if k else own_pool)[:, columns]
        for g in range(0, len(chunks), 2):
            some = min(2, len(chunks) - g)
            got = dot(select[k, g * chunk : (g + some) * chunk, :], pool).astype(jnp.bfloat16)
            for i in range(some):
                for b in range(blocks):
                    at = (b * NC + k) * chunk
                    outs[g + i][at : at + chunk, :] = got[i * chunk : (i + 1) * chunk, b * LANES : (b + 1) * LANES]


def add_up(most, kinds2, ins, h, before=None):
    chunk = N * ZH * NC * most
    blocks = (ins[0].shape[0] - TILE) // (NC * chunk)
    lines = chunk // LANES
    segments = LANES // most * kinds2
    row = iota((segments, LANES), 0)
    base = lax.div(iota((1, LANES), 1), most) * kinds2 - 1
    ones = jnp.ones((TILE, 2 * NC * LANES), jnp.bfloat16)
    sums, count = before if before is not None else (0.0, 0.0)
    for j in range(0, len(ins), 2):
        hots, data = [], []
        for r in ins[j : j + 2]:
            labels = r[blocks * NC * chunk :, :].astype(jnp.float32).astype(jnp.int32)
            for k in range(NC):
                label = labels[k * lines + h : k * lines + h + 1]
                hots.append(one_hot(row == jnp.where(label > 0, base + label, -1)))
                first = [(b * NC + k) * chunk + h * LANES for b in range(blocks)]
                data.append(jnp.concatenate([r[i : i + LANES, :] for i in first], axis=1))
        hot = jnp.concatenate(hots, axis=1)
        sums = sums + dot(hot, jnp.concatenate(data, axis=0))
        count = count + dot(ones, hot, ((1,), (1,)))
    return sums, count


def early_kernel(most, kinds2, *rest):
    ins, (total, tally) = rest[:-2], rest[-2:]
    lines = tally.shape[0]
    segments = total.shape[0] // lines
    for h in range(lines):
        total[h * segments : (h + 1) * segments, :], tally[h] = add_up(most, kinds2, ins, h)


def late_kernel(most, kinds2, sum_ref, tally_ref, *rest):
    ins, outs = rest[:-N], rest[-N:]
    lines = tally_ref.shape[0]
    segments = sum_ref.shape[0] // lines
    blocks = sum_ref.shape[1] // LANES
    part = lines * segments // N
    for h in range(lines):
        before = (sum_ref[h * segments : (h + 1) * segments, :], tally_ref[h])
        sums, count = add_up(most, kinds2, ins, h, before)
        for p in range(segments // part):
            out = outs[CROSS.index(h * (segments // part) + p)]
            for k in range(blocks):
                out[k * part : (k + 1) * part, :] = sums[p * part : (p + 1) * part, k * LANES : (k + 1) * LANES]
            out[blocks * part :, :] = count[:, p * part : (p + 1) * part]


def cross_kernel(*rest):
    ins, outs = rest[:N], rest[N:]
    part = outs[0].shape[0] - TILE
    blocks = (ins[0].shape[0] - TILE) // LANES
    some = part // blocks
    total = (ins[0][...] + ins[1][...]) + (ins[2][...] + ins[3][...])
    for step, out in zip(DEEP, outs):
        for k in range(blocks):
            out[k * some : (k + 1) * some, :] = total[k * LANES + step * some : k * LANES + (step + 1) * some]
        tile = total[blocks * LANES :]
        out[part:, :] = jnp.concatenate([tile[:, step * some :], tile[:, : step * some]], axis=1) if step else tile


def depth_kernel(some, *rest):
    ins, (other_ref, mine_ref) = rest[:ZH], rest[ZH:]
    total = (ins[0][...] + ins[1][...]) + (ins[2][...] + ins[3][...])
    part = other_ref.shape[0]
    for side, out in enumerate((mine_ref, other_ref)):
        for k in range(part // some):
            at = (k * NC + side) * some
            out[k * some : (k + 1) * some, :] = total[at : at + some]
    mine_ref[part:, :] = total[NC * part :]


def finish_kernel(kinds, where, old_ref, mine_ref, came_ref, out):
    half, width = came_ref.shape[0], old_ref.shape[1]
    core = where[4]
    blocks = width // LANES
    part = 2 * half // blocks
    lane = iota((part, LANES), 1)
    here = lane == iota((part, LANES), 0)
    count = jnp.sum(jnp.where(here, mine_ref[half : half + 1, :], 0.0), axis=1, keepdims=True)
    divisor = jnp.broadcast_to(count + 1.0, (part, LANES))
    rows = pl.ds(pl.multiple_of(where[5] * part, part), part)
    for k in range(blocks):
        at = slice(k * LANES, (k + 1) * LANES)
        rest = slice(k % (blocks // NC) * part, (k % (blocks // NC) + 1) * part)
        total = jnp.where(core == k // (blocks // NC), mine_ref[rest, :], came_ref[rest, :])
        out[:, at] = (total + old_ref[rows, at]) / divisor
    count = jnp.where(lane == lax.rem(iota((part, LANES), 0), kinds), count, 0.0)
    line = iota((part, LANES), 0)
    tile = jnp.zeros((part, LANES), jnp.float32)
    for k in range(part // kinds):
        tile = jnp.where(line == k, jnp.sum(count[k * kinds : (k + 1) * kinds], axis=0, keepdims=True), tile)
    out[:, width:] = tile


def place_kernel(where, *rest):
    ins, (fresh_ref, count_ref) = rest[:-2], rest[-2:]
    part, width = ins[0].shape[0], fresh_ref.shape[1]
    kinds = count_ref.shape[1]
    for step, r in zip(TURNS, ins):
        q = lax.rem(where[5] - step + N, N)
        fresh_ref[pl.ds(pl.multiple_of(q * part, part), part), :] = r[:, :width]
        for k in range(part // kinds):
            line = r[k : k + 1, width : width + kinds]
            count_ref[pl.ds(q * (part // kinds) + k, 1), :] = line.astype(jnp.int32)


def per_device(pool_rows, sample_index, cluster_id, child_id, old_centroids):
    rows, width = pool_rows.shape
    block, kinds = old_centroids.shape[:2]
    owned = block // N
    most = 4 * rows // (block * N * NZ * NC)
    half = width // NC
    blocks = half // LANES
    chunk = N * NZ * NC * N * most // CHUNKS
    part = owned * kinds
    y, x, zh, zl, c = (lax.axis_index(a) for a in AXES)
    where = jnp.stack([x + (y - x) * c, y + (x - y) * c, zl, zh, c, y])

    def other_core(y, x, z, c):
        return y, x, z, 1 - c

    ints = jnp.stack([sample_index, cluster_id, child_id]).reshape(3, 1, rows)
    came_ints = permute(ints, other_core)
    came_pool = permute(pool_rows, other_core)
    slots = CHUNKS * chunk
    lines = [shape(slots // most, most), shape(slots // LANES, LANES)]
    own_lines = call(functools.partial(lines_kernel, most, owned, kinds), lines, [SMEM, VMEM], [where, ints])
    *came_lines, own_pool = call(
        functools.partial(pool_kernel, most, owned, kinds),
        [*lines, shape(rows, width, dtype=jnp.bfloat16)],
        [SMEM, VMEM, HBM],
        [where, came_ints, pltpu.with_memory_space_constraint(pool_rows, HBM)],
        [DMA],
    )
    came = []
    for moves in (RAW[:FIRST], RAW[FIRST:] + [(0, 0)]):
        packed = call(
            functools.partial(fill_kernel, [step * ZL + swap for step, swap in moves]),
            [shape(blocks * NC * chunk + TILE, LANES, dtype=jnp.bfloat16)] * len(moves),
            [SMEM] + [VMEM] * 6,
            [where, *own_lines, *came_lines, own_pool, came_pool],
            [VMEM((NC, len(moves) * chunk, rows), jnp.bfloat16)],
        )
        came += [permute(p, raw_move(*move)) if any(move) else p for p, move in zip(packed, moves)]
    segments = N * ZH * NC * part
    sums = [shape(segments, half), shape(chunk // LANES, TILE, segments * LANES // chunk)]
    early = call(functools.partial(early_kernel, most, part), sums, [VMEM] * EARLY, came[:EARLY])
    pieces = call(
        functools.partial(late_kernel, most, part),
        [shape(blocks * segments // N + TILE, LANES)] * N,
        [VMEM] * (2 + CHUNKS - EARLY),
        [*early, *came[EARLY:]],
    )
    pieces = [pieces[0]] + [permute(p, cross_move(t)) for t, p in zip(CROSS[1:], pieces[1:])]
    pieces = call(cross_kernel, [shape(blocks * NC * part + TILE, LANES)] * ZH, [VMEM] * N, pieces)
    pieces = [pieces[0]] + [
        permute(p, lambda y, x, z, c, t=t: (y, x, z + ZL * t, c)) for t, p in zip(DEEP[1:], pieces[1:])
    ]
    other, mine = call(
        functools.partial(depth_kernel, part),
        [shape(blocks * part, LANES), shape(blocks * part + TILE, LANES)],
        [VMEM] * ZH,
        pieces,
    )
    fresh = call(
        functools.partial(finish_kernel, kinds),
        shape(part, width + LANES),
        [SMEM, VMEM, VMEM, VMEM],
        [where, old_centroids.reshape(block * kinds, width), mine, permute(other, other_core)],
    )
    quarters = [fresh]
    for t in TURNS[1:]:
        quarters.append(permute(fresh, lambda y, x, z, c, t=t: (y + t, x, z, c)))
    centroids, counts = call(
        place_kernel,
        [shape(block * kinds, width), shape(block, kinds, dtype=jnp.int32)],
        [SMEM] + [VMEM] * N,
        [where, *quarters],
    )
    return centroids.reshape(block, kinds, width), counts


def solution(mesh):
    fine = Mesh(mesh.devices.reshape(SIZES), AXES)
    dev = ("x", "zh", "zl", "c")
    placed = (P(AXES, None), P(AXES), P(AXES), P(AXES), P(dev, None, None))

    return jax.shard_map(
        per_device,
        mesh=fine,
        in_specs=placed,
        out_specs=(P(dev, None, None), P(dev, None)),
        check_vma=False,
    )
```

```python
import functools

import jax
import jax.numpy as jnp
from jax import lax
from jax.experimental import pallas as pl
from jax.experimental.pallas import tpu as pltpu
from jax.sharding import Mesh, PartitionSpec as P


AXES = ("y", "x", "zh", "zl", "c")
SIZES = (4, 4, 4, 2, 2)
N, ZH, ZL, NC = 4, 4, 2, 2
NZ = ZH * ZL
CHUNKS = N * ZL
LANES = 128
TILE = 8
LOW = 32
VMEM = pltpu.VMEM
SMEM = pltpu.SMEM
HBM = pltpu.HBM
DMA = pltpu.SemaphoreType.DMA

RAW = [(2, 1), (2, 0), (0, 1), (1, 1), (3, 0), (3, 1), (1, 0)]
FIRST = 3
CROSS = [0, 2, 1, 3]
DEEP = [0, 2, 1, 3]
TURNS = [0, 2, 1, 3]
EARLY = 4


def permute(value, move):
    pairs = []
    for y in range(N):
        for x in range(N):
            for z in range(NZ):
                for c in range(NC):
                    ty, tx, tz, tc = move(y, x, z, c)
                    to = (((ty % N) * N + tx % N) * NZ + tz % NZ) * NC + tc % NC
                    pairs.append((((y * N + x) * NZ + z) * NC + c, to))
    return lax.ppermute(value, AXES, pairs)


def raw_move(step, swap):
    def move(y, x, z, c):
        if swap:
            z = z ^ 1 if c == 0 else (z + 1 if z % 2 else z - 1)
        return (y, x + step, z, c) if c == 0 else (y + step, x, z, c)

    return move


def cross_move(step):
    return lambda y, x, z, c: (y + step, x, z, c) if c == 0 else (y, x + step, z, c)


def iota(shape, dim):
    return lax.broadcasted_iota(jnp.int32, shape, dim)


def one_hot(mask, dtype=jnp.bfloat16):
    return jnp.where(mask, 1.0, 0.0).astype(dtype)


def dot(a, b, dims=((1,), (0,))):
    return lax.dot_general(a, b, (dims, ((), ())), preferred_element_type=jnp.float32)


def shape(*dims, dtype=jnp.float32):
    return jax.ShapeDtypeStruct(dims, dtype)


def call(kernel, outs, spaces, args, scratch=(), places=None):
    return pl.pallas_call(
        kernel,
        out_shape=outs,
        in_specs=[pl.BlockSpec(memory_space=s) for s in spaces],
        out_specs=places or jax.tree.map(lambda _: pl.BlockSpec(memory_space=VMEM), outs),
        scratch_shapes=list(scratch),
        compiler_params=pltpu.CompilerParams(vmem_limit_bytes=44 << 20),
    )(*args)


def ranks(hot, mask):
    owners, rows = hot.shape
    wide = (LANES, 2 * LANES)
    before = one_hot((iota(wide, 0) < iota(wide, 1)) | (iota(wide, 1) >= LANES))
    seen = jnp.zeros((owners, LANES), jnp.float32)
    out = []
    for b in range(rows // LANES):
        at = slice(b * LANES, (b + 1) * LANES)
        counted = dot(hot[:, at], before)
        out.append(jnp.sum(jnp.where(mask[:, at], counted[:, :LANES] + seen, 0.0), axis=0, keepdims=True))
        seen = seen + counted[:, LANES:]
    return jnp.concatenate(out, axis=1).astype(jnp.int32)


def lines_of(where, most, owned, kinds, ints):
    a_me, b_me, odd, z_me, core = where[0], where[1], where[2], where[3], where[4]
    rows = ints.shape[2]
    index, cluster, child = ints[0], ints[1], ints[2]
    owner = lax.div(cluster, owned)
    quarter = lax.rem(owner, N)
    dev = lax.div(owner, N)
    to_core = lax.rem(dev, NC)
    z = lax.rem(lax.div(dev, NC), NZ)
    x = lax.div(dev, NC * NZ)
    a = x + (quarter - x) * core
    b = quarter + (x - quarter) * core
    step = lax.rem(a - a_me + N, N)
    swap = lax.rem(lax.rem(z, ZL) + odd, ZL)
    b = lax.rem(b - b_me + N, N)
    pair = lax.rem(lax.div(z, ZL) - z_me + swap * core * (1 - 2 * odd) + 2 * ZH, ZH)
    spot = ((step * ZL + swap) * N + b) * (ZH * NC) + pair * NC + lax.rem(to_core + core, NC)
    spots = N * N * NZ * NC
    mask = iota((spots, rows), 0) == spot
    hot = one_hot(mask)
    rank = iota((most, rows), 0) == ranks(hot, mask)
    index = lax.rem(index, rows) + 1
    label = lax.rem(cluster, owned) * kinds + child + 1

    high = lax.div(index, LOW)
    lines = [jnp.where(rank, a.astype(jnp.float32), 0.0) for a in (index - high * LOW, high * LOW, label)]
    spread = dot(hot, jnp.concatenate(lines, axis=0).astype(jnp.bfloat16), ((1,), (1,)))
    source = spread[:, :most] + spread[:, most : 2 * most]
    per = LANES // most
    tile = one_hot(iota((most, LANES), 0) == lax.rem(iota((most, LANES), 1), most))
    label = dot(spread[:, 2 * most :].astype(jnp.bfloat16), tile)
    keep = lax.div(iota((spots, LANES), 1), most) == lax.rem(iota((spots, LANES), 0), per)
    label = jnp.sum(jnp.where(keep, label, 0.0).reshape(spots // per, per, LANES), axis=1)
    return source, label


def lines_kernel(most, owned, kinds, where, ints_ref, source_ref, label_ref):
    source_ref[...], label_ref[...] = lines_of(where, most, owned, kinds, ints_ref)


def pool_kernel(most, owned, kinds, where, ints_ref, pool_hbm, source_ref, label_ref, pool, sem):
    copy = pltpu.make_async_copy(pool_hbm, pool, sem)
    copy.start()
    source_ref[...], label_ref[...] = lines_of(where, most, owned, kinds, ints_ref)
    copy.wait()


def fill_kernel(chunks, where, own_source, own_label, came_source, came_label, own_pool, came_pool, *rest):
    outs, select = rest[:-1], rest[-1]
    rows, width = own_pool.shape[0], own_pool.shape[1] // NC
    blocks = width // LANES
    most = own_source.shape[1]
    spots = own_source.shape[0] // CHUNKS
    chunk = spots * most
    pick = iota((chunk, most), 1) == lax.rem(iota((chunk, most), 0), most)
    lines = chunk // LANES
    line = iota((TILE, LANES), 0)
    for i, j in enumerate(chunks):
        tile = jnp.zeros((TILE, LANES), jnp.float32)
        for k, (source_ref, label_ref) in enumerate(((own_source, own_label), (came_source, came_label))):
            source = source_ref[j * spots : (j + 1) * spots, :]
            source = jnp.broadcast_to(source[:, None, :], (spots, most, most)).reshape(chunk, most)
            source = jnp.sum(jnp.where(pick, source, 0.0), axis=1, keepdims=True).astype(jnp.int32)
            select[k, i * chunk : (i + 1) * chunk, :] = one_hot(iota((chunk, rows), 1) + 1 == source)
            for h in range(lines):
                tile = jnp.where(line == k * lines + h, label_ref[j * lines + h : j * lines + h + 1, :], tile)
        outs[i][blocks * NC * chunk :, :] = tile.astype(jnp.bfloat16)
    columns = pl.ds(pl.multiple_of(where[4] * width, width), width)
    for k in range(NC):
        pool = (came_pool if k else own_pool)[:, columns]
        for g in range(0, len(chunks), 2):
            some = min(2, len(chunks) - g)
            got = dot(select[k, g * chunk : (g + some) * chunk, :], pool).astype(jnp.bfloat16)
            for i in range(some):
                for b in range(blocks):
                    at = (b * NC + k) * chunk
                    outs[g + i][at : at + chunk, :] = got[i * chunk : (i + 1) * chunk, b * LANES : (b + 1) * LANES]


def add_up(most, kinds2, ins, h, before=None):
    chunk = N * ZH * NC * most
    blocks = (ins[0].shape[0] - TILE) // (NC * chunk)
    lines = chunk // LANES
    segments = LANES // most * kinds2
    row = iota((segments, LANES), 0)
    base = lax.div(iota((1, LANES), 1), most) * kinds2 - 1
    ones = jnp.ones((TILE, 2 * NC * LANES), jnp.bfloat16)
    sums, count = before if before is not None else (0.0, 0.0)
    for j in range(0, len(ins), 2):
        hots, data = [], []
        for r in ins[j : j + 2]:
            labels = r[blocks * NC * chunk :, :].astype(jnp.float32).astype(jnp.int32)
            for k in range(NC):
                label = labels[k * lines + h : k * lines + h + 1]
                hots.append(one_hot(row == jnp.where(label > 0, base + label, -1)))
                first = [(b * NC + k) * chunk + h * LANES for b in range(blocks)]
                data.append(jnp.concatenate([r[i : i + LANES, :] for i in first], axis=1))
        hot = jnp.concatenate(hots, axis=1)
        sums = sums + dot(hot, jnp.concatenate(data, axis=0))
        count = count + dot(ones, hot, ((1,), (1,)))
    return sums, count


def early_kernel(most, kinds2, *rest):
    ins, (total, tally) = rest[:-2], rest[-2:]
    lines = tally.shape[0]
    segments = total.shape[0] // lines
    for h in range(lines):
        total[h * segments : (h + 1) * segments, :], tally[h] = add_up(most, kinds2, ins, h)


def late_kernel(most, kinds2, sum_ref, tally_ref, *rest):
    ins, outs = rest[:-N], rest[-N:]
    lines = tally_ref.shape[0]
    segments = sum_ref.shape[0] // lines
    blocks = sum_ref.shape[1] // LANES
    part = lines * segments // N
    for h in range(lines):
        before = (sum_ref[h * segments : (h + 1) * segments, :], tally_ref[h])
        sums, count = add_up(most, kinds2, ins, h, before)
        for p in range(segments // part):
            out = outs[CROSS.index(h * (segments // part) + p)]
            for k in range(blocks):
                out[k * part : (k + 1) * part, :] = sums[p * part : (p + 1) * part, k * LANES : (k + 1) * LANES]
            out[blocks * part :, :] = count[:, p * part : (p + 1) * part]


def cross_kernel(*rest):
    ins, outs = rest[:N], rest[N:]
    part = outs[0].shape[0] - TILE
    blocks = (ins[0].shape[0] - TILE) // LANES
    some = part // blocks
    total = (ins[0][...] + ins[1][...]) + (ins[2][...] + ins[3][...])
    for step, out in zip(DEEP, outs):
        for k in range(blocks):
            out[k * some : (k + 1) * some, :] = total[k * LANES + step * some : k * LANES + (step + 1) * some]
        tile = total[blocks * LANES :]
        out[part:, :] = jnp.concatenate([tile[:, step * some :], tile[:, : step * some]], axis=1) if step else tile


def depth_kernel(some, *rest):
    ins, (other_ref, mine_ref) = rest[:ZH], rest[ZH:]
    total = (ins[0][...] + ins[1][...]) + (ins[2][...] + ins[3][...])
    part = other_ref.shape[0]
    for side, out in enumerate((mine_ref, other_ref)):
        for k in range(part // some):
            at = (k * NC + side) * some
            out[k * some : (k + 1) * some, :] = total[at : at + some]
    mine_ref[part:, :] = total[NC * part :]


def finish_kernel(kinds, where, old_ref, mine_ref, came_ref, out):
    half, width = came_ref.shape[0], old_ref.shape[1]
    core = where[4]
    blocks = width // LANES
    part = 2 * half // blocks
    lane = iota((part, LANES), 1)
    here = lane == iota((part, LANES), 0)
    count = jnp.sum(jnp.where(here, mine_ref[half : half + 1, :], 0.0), axis=1, keepdims=True)
    divisor = jnp.broadcast_to(count + 1.0, (part, LANES))
    rows = pl.ds(pl.multiple_of(where[5] * part, part), part)
    for k in range(blocks):
        at = slice(k * LANES, (k + 1) * LANES)
        rest = slice(k % (blocks // NC) * part, (k % (blocks // NC) + 1) * part)
        total = jnp.where(core == k // (blocks // NC), mine_ref[rest, :], came_ref[rest, :])
        out[:, at] = (total + old_ref[rows, at]) / divisor
    count = jnp.where(lane == lax.rem(iota((part, LANES), 0), kinds), count, 0.0)
    line = iota((part, LANES), 0)
    tile = jnp.zeros((part, LANES), jnp.float32)
    for k in range(part // kinds):
        tile = jnp.where(line == k, jnp.sum(count[k * kinds : (k + 1) * kinds], axis=0, keepdims=True), tile)
    out[:, width:] = tile


def place_kernel(where, *rest):
    ins, (fresh_hbm, count_ref, fresh, sems) = rest[:-4], rest[-4:]
    part, width = ins[0].shape[0], fresh.shape[2]
    kinds = count_ref.shape[1]
    copies = []
    for j, (step, r) in enumerate(zip(TURNS, ins)):
        q = lax.rem(where[5] - step + N, N)
        fresh[j] = r[:, :width]
        rows = pl.ds(pl.multiple_of(q * part, part), part)
        copies.append(pltpu.make_async_copy(fresh.at[j], fresh_hbm.at[rows, :], sems.at[j]))
        copies[-1].start()
        for k in range(part // kinds):
            line = r[k : k + 1, width : width + kinds]
            count_ref[pl.ds(q * (part // kinds) + k, 1), :] = line.astype(jnp.int32)
    for copy in copies:
        copy.wait()


def per_device(pool_rows, sample_index, cluster_id, child_id, old_centroids):
    rows, width = pool_rows.shape
    block, kinds = old_centroids.shape[:2]
    owned = block // N
    most = 4 * rows // (block * N * NZ * NC)
    half = width // NC
    blocks = half // LANES
    chunk = N * NZ * NC * N * most // CHUNKS
    part = owned * kinds
    y, x, zh, zl, c = (lax.axis_index(a) for a in AXES)
    where = jnp.stack([x + (y - x) * c, y + (x - y) * c, zl, zh, c, y])

    def other_core(y, x, z, c):
        return y, x, z, 1 - c

    ints = jnp.stack([sample_index, cluster_id, child_id]).reshape(3, 1, rows)
    came_ints = permute(ints, other_core)
    came_pool = permute(pool_rows, other_core)
    slots = CHUNKS * chunk
    lines = [shape(slots // most, most), shape(slots // LANES, LANES)]
    own_lines = call(functools.partial(lines_kernel, most, owned, kinds), lines, [SMEM, VMEM], [where, ints])
    *came_lines, own_pool = call(
        functools.partial(pool_kernel, most, owned, kinds),
        [*lines, shape(rows, width, dtype=jnp.bfloat16)],
        [SMEM, VMEM, HBM],
        [where, came_ints, pltpu.with_memory_space_constraint(pool_rows, HBM)],
        [DMA],
    )
    came = []
    for moves in (RAW[:FIRST], RAW[FIRST:] + [(0, 0)]):
        packed = call(
            functools.partial(fill_kernel, [step * ZL + swap for step, swap in moves]),
            [shape(blocks * NC * chunk + TILE, LANES, dtype=jnp.bfloat16)] * len(moves),
            [SMEM] + [VMEM] * 6,
            [where, *own_lines, *came_lines, own_pool, came_pool],
            [VMEM((NC, len(moves) * chunk, rows), jnp.bfloat16)],
        )
        came += [permute(p, raw_move(*move)) if any(move) else p for p, move in zip(packed, moves)]
    segments = N * ZH * NC * part
    sums = [shape(segments, half), shape(chunk // LANES, TILE, segments * LANES // chunk)]
    early = call(functools.partial(early_kernel, most, part), sums, [VMEM] * EARLY, came[:EARLY])
    pieces = call(
        functools.partial(late_kernel, most, part),
        [shape(blocks * segments // N + TILE, LANES)] * N,
        [VMEM] * (2 + CHUNKS - EARLY),
        [*early, *came[EARLY:]],
    )
    pieces = [pieces[0]] + [permute(p, cross_move(t)) for t, p in zip(CROSS[1:], pieces[1:])]
    pieces = call(cross_kernel, [shape(blocks * NC * part + TILE, LANES)] * ZH, [VMEM] * N, pieces)
    pieces = [pieces[0]] + [
        permute(p, lambda y, x, z, c, t=t: (y, x, z + ZL * t, c)) for t, p in zip(DEEP[1:], pieces[1:])
    ]
    other, mine = call(
        functools.partial(depth_kernel, part),
        [shape(blocks * part, LANES), shape(blocks * part + TILE, LANES)],
        [VMEM] * ZH,
        pieces,
    )
    fresh = call(
        functools.partial(finish_kernel, kinds),
        shape(part, width + LANES),
        [SMEM, VMEM, VMEM, VMEM],
        [where, old_centroids.reshape(block * kinds, width), mine, permute(other, other_core)],
    )
    quarters = [fresh]
    for t in TURNS[1:]:
        quarters.append(permute(fresh, lambda y, x, z, c, t=t: (y + t, x, z, c)))
    centroids, counts = call(
        place_kernel,
        [shape(block * kinds, width), shape(block, kinds, dtype=jnp.int32)],
        [SMEM] + [VMEM] * N,
        [where, *quarters],
        [VMEM((N, part, width), jnp.float32), DMA((N,))],
        [pl.BlockSpec(memory_space=HBM), pl.BlockSpec(memory_space=VMEM)],
    )
    return centroids.reshape(block, kinds, width), counts


def solution(mesh):
    fine = Mesh(mesh.devices.reshape(SIZES), AXES)
    dev = ("x", "zh", "zl", "c")
    placed = (P(AXES, None), P(AXES), P(AXES), P(AXES), P(dev, None, None))

    return jax.shard_map(
        per_device,
        mesh=fine,
        in_specs=placed,
        out_specs=(P(dev, None, None), P(dev, None)),
        check_vma=False,
    )
```
